256 devices in a mesh: energy: 16 (over x, z_lo, core), kpt: 4 (over z_hi), layer: 4 (over y).
Axes of the slice: x: 4, y: 4, z: 8 (z_hi: 4, z_lo: 2; z = z_hi * 2 + z_lo), core: 2. Of those that a mesh axis runs over, the one named last changes fastest.
Arguments:
- energies: float32 [64], P(('energy', 'layer')), may hold values from -1.5 to 1.5
- momenta: float32 [4], P('kpt'), may hold values from 0 to 1
- energy_level: int32 [64], P(('energy', 'layer')), may hold values from 0 to 7
- momentum_level: int32 [4], P('kpt'), may hold values from 0 to 7
- energy_table: float32 [8], replicated, may hold values from 0.25 to 4
- momentum_table: float32 [8], replicated, may hold values from 0.25 to 4
- onsite: float32 [5, 256, 256], replicated, may hold values from -1 to 1, as said below
- broad: float32 [5, 256], replicated, may hold values from 1 to 4
- kdiag: float32 [5, 256], replicated, may hold values from 0.2 to 2
- fermi: float32 [5], replicated, may hold values from -1 to 1
- couplings: float32 [3, 256, 256], replicated, may hold values from -0.0624 to 0.0624
- bond_kind: int32 [4], replicated, may hold values from 0 to 2
Outputs:
- density: float32 [4, 2, 256, 256], P('layer', None, 'energy')
- current: float32 [4, 2, 256, 256], P('layer', None, 'energy')
The draws below stay inside these ranges and needn't reach their ends.
Inputs may be any that keep to these rules, and one draw needn't show every extreme that they name: Each block of onsite is symmetric.
All inputs are finite; a program needn't handle non-finite values.
Results may differ from the reference program's by a relative error of at most 0.0001.
Values sent between devices are 32-bit elements; how exact they have to be, the bound alone decides.
A program may use at most 64 MiB of HBM per device.

```python
import math
import jax
import jax.numpy as jnp
from jax import lax

B = 256
NKIND = 3
LEVELS = 8
NL = 4
NLS = 5
NE = 64
NK = 4


def draw_onsite(key, part):
    first_key, second_key = jax.random.split(jax.random.fold_in(key, 17))
    raw = jax.random.normal(first_key, (NLS, B, B), jnp.float32) * 0.0069
    symmetric = (raw + jnp.swapaxes(raw, 1, 2)) * 0.7071
    levels = jax.random.uniform(second_key, (NLS, B), jnp.float32, -1.0, 1.0)
    identity = jnp.eye(B, dtype=jnp.float32)
    return symmetric * (1.0 - identity) + levels[:, :, None] * identity


def place_ends(result, stream_key, low, high):
    dims = result.shape
    spot = [jax.random.randint(jax.random.fold_in(stream_key, axis), (), 0, dims[axis]) for axis in range(len(dims))]
    result = result.at[tuple(spot)].set(low)
    longest = dims.index(max(dims))
    spot[longest] = (spot[longest] + 1) % dims[longest]
    return result.at[tuple(spot)].set(high)


def level_of(stream_key, dims, shards, low, high):
    def one(position, shards_of):
        steps = jax.random.uniform(jax.random.fold_in(jax.random.fold_in(stream_key, 6), position), (shards_of,), jnp.float32, low / len(shards), high / len(shards))
        return jnp.repeat(jnp.exp(steps), dims[position] // shards_of).reshape((-1,) + (1,) * (len(dims) - position - 1))

    loudness = one(*shards[0])
    for cut in shards[1:]:
        loudness = loudness * one(*cut)
    return loudness


def normal_values(rng, extent, width, reach, held_as=jnp.bfloat16):
    result = jax.random.normal(rng, extent, jnp.float32) * width
    return jnp.minimum(jnp.maximum(result, -reach), reach).astype(held_as)


def setup_inputs(seed: int = 0) -> dict:
    arg_keys = jax.random.split(jax.random.key(seed), 13)
    return {
        "energies": jnp.clip(jax.random.uniform(arg_keys[0], (NE,), jnp.float32, -1.5, 1.5) * level_of(arg_keys[0], (NE,), ((0, 64),), -0.4, 0.0), -1.5, 1.5),
        "momenta": jnp.clip(1.0 * jax.random.uniform(arg_keys[1], (NK,), jnp.float32) ** level_of(arg_keys[1], (NK,), ((0, 4),), -0.2, 0.2), 0.0, 1.0),
        "energy_level": place_ends(jax.random.randint(arg_keys[2], (NE,), 0, LEVELS), jax.random.fold_in(arg_keys[2], 1), 0, LEVELS - 1).astype(jnp.int32),
        "momentum_level": place_ends(jax.random.randint(arg_keys[3], (NK,), 0, LEVELS), jax.random.fold_in(arg_keys[3], 1), 0, LEVELS - 1).astype(jnp.int32),
        "energy_table": jnp.clip(jnp.exp(jax.random.uniform(arg_keys[4], (LEVELS,), jnp.float32, math.log(0.25), math.log(4.0))), 0.25, 4.0),
        "momentum_table": jnp.clip(jnp.exp(jax.random.uniform(arg_keys[5], (LEVELS,), jnp.float32, math.log(0.25), math.log(4.0))), 0.25, 4.0),
        "onsite": draw_onsite(jax.random.fold_in(arg_keys[12], 71), 0),
        "broad": jnp.clip(jnp.exp(jax.random.uniform(arg_keys[7], (NLS, B), jnp.float32, math.log(1.0), math.log(4.0))), 1.0, 4.0),
        "kdiag": jnp.clip(jnp.exp(jax.random.uniform(arg_keys[8], (NLS, B), jnp.float32, math.log(0.2), math.log(2.0))), 0.2, 2.0),
        "fermi": jnp.clip(jax.random.uniform(arg_keys[9], (NLS,), jnp.float32, -1.0, 1.0), -1.0, 1.0),
        "couplings": normal_values(arg_keys[10], (NKIND, B, B), 0.0104, 0.0624, jnp.float32),
        "bond_kind": place_ends(jax.random.randint(arg_keys[11], (NL,), 0, NKIND), jax.random.fold_in(arg_keys[11], 1), 0, NKIND - 1).astype(jnp.int32),
    }


exact_mode = lax.Precision.HIGHEST
thermal = 0.25


def real_dot(left, right):
    return jnp.matmul(left, right, precision=exact_mode)


def complex_dot(left, right):
    return (real_dot(left[0], right[0]) - real_dot(left[1], right[1]),
            real_dot(left[0], right[1]) + real_dot(left[1], right[0]))


def real_left(matrix, values):
    return (real_dot(matrix, values[0]), real_dot(matrix, values[1]))


def real_right(values, matrix):
    return (real_dot(values[0], matrix), real_dot(values[1], matrix))


def swap_last(array):
    return jnp.swapaxes(array, -1, -2)


def adjoint(values):
    return (swap_last(values[0]), -swap_last(values[1]))


def transpose_pair(values):
    return (swap_last(values[0]), swap_last(values[1]))


def diag_embed(vector):
    return vector[..., :, None] * jnp.eye(vector.shape[-1], dtype=vector.dtype)


def invert(matrix):
    diag_real = jnp.diagonal(matrix[0], axis1=-2, axis2=-1)
    diag_imag = jnp.diagonal(matrix[1], axis1=-2, axis2=-1)
    modulus = diag_real * diag_real + diag_imag * diag_imag
    start_real = diag_real / modulus
    start_imag = -diag_imag / modulus
    scaled_real = start_real[..., :, None] * matrix[0] - start_imag[..., :, None] * matrix[1]
    scaled_imag = start_real[..., :, None] * matrix[1] + start_imag[..., :, None] * matrix[0]
    both_real = scaled_real * start_real[..., None, :] - scaled_imag * start_imag[..., None, :]
    both_imag = scaled_real * start_imag[..., None, :] + scaled_imag * start_real[..., None, :]
    first = (2.0 * diag_embed(start_real) - both_real, 2.0 * diag_embed(start_imag) - both_imag)
    second = complex_dot(first, complex_dot(matrix, first))
    return (2.0 * first[0] - second[0], 2.0 * first[1] - second[1])


def forward_sweep(energy_pts, moment_pts, onsite, broad, kdiag, fermi, bonds):
    greens = []
    lessers = []
    for layer_at in range(onsite.shape[0]):
        shift = energy_pts[:, None] - moment_pts[:, None] * kdiag[layer_at][None, :]
        base_real = diag_embed(shift) - onsite[layer_at]
        base_imag = diag_embed(jnp.broadcast_to(0.5 * broad[layer_at], shift.shape))
        source = broad[layer_at][None, :] * jax.nn.sigmoid((fermi[layer_at] - energy_pts[:, None]) / thermal)
        if layer_at == 0:
            green = invert((base_real, base_imag))
            scaled = (green[0] * source[:, None, :], green[1] * source[:, None, :])
            lesser = complex_dot(scaled, adjoint(green))
        else:
            bond = bonds[layer_at - 1]
            self_part = real_right(real_left(swap_last(bond), greens[-1]), bond)
            green = invert((base_real - self_part[0], base_imag - self_part[1]))
            inflow = real_right(real_left(swap_last(bond), lessers[-1]), bond)
            lesser = complex_dot(complex_dot(green, (inflow[0] + diag_embed(source), inflow[1])), adjoint(green))
        greens.append(green)
        lessers.append(lesser)
    return greens, lessers


def backward_step(green, lesser, bond, right_green, right_lesser):
    hopping = real_right(green, bond)
    carried = complex_dot(hopping, right_green)
    spread_green = complex_dot(carried, transpose_pair(hopping))
    new_green = (green[0] + spread_green[0], green[1] + spread_green[1])
    hop_lesser = complex_dot(hopping, right_lesser)
    through = complex_dot(right_green, real_left(swap_last(bond), lesser))
    cross = complex_dot(hopping, through)
    cross_adj = adjoint(cross)
    spread = complex_dot(hop_lesser, adjoint(hopping))
    new_lesser = (lesser[0] + spread[0] + cross[0] + cross_adj[0],
                  lesser[1] + spread[1] + cross[1] + cross_adj[1])
    through_adj = adjoint(through)
    current = (hop_lesser[0] + through_adj[0], hop_lesser[1] + through_adj[1])
    return new_green, new_lesser, current


def weighted_sum(weights, values):
    return jnp.stack([jnp.tensordot(weights, values[0], axes=1, precision=exact_mode),
                      jnp.tensordot(weights, values[1], axes=1, precision=exact_mode)])


def pick_rows(levels, table):
    count = table.shape[0]
    onehot = (levels[:, None] == jnp.arange(count, dtype=jnp.int32)[None, :]).astype(table.dtype)
    return jnp.sum(onehot * table[None, :], axis=1)


def reference(energies, momenta, energy_level, momentum_level, energy_table, momentum_table, onsite, broad, kdiag, fermi, couplings, bond_kind):
    kinds = couplings.shape[0]
    choose = (bond_kind[:, None] == jnp.arange(kinds, dtype=jnp.int32)[None, :]).astype(couplings.dtype)
    bonds = jnp.tensordot(choose, couplings, axes=1, precision=exact_mode)
    energy_weight = pick_rows(energy_level, energy_table)
    moment_weight = pick_rows(momentum_level, momentum_table)
    scale = 1.0 / (NE * NK)
    layers = onsite.shape[0] - 1

    def accumulate(carry, index):
        energy_pts = jnp.broadcast_to(energies[index], momenta.shape)
        weights = energy_weight[index] * moment_weight * scale
        greens, lessers = forward_sweep(energy_pts, momenta, onsite, broad, kdiag, fermi, bonds)
        right_green = greens[layers]
        right_lesser = lessers[layers]
        density_rows = [None] * layers
        current_rows = [None] * layers
        for layer_at in range(layers - 1, -1, -1):
            right_green, right_lesser, current = backward_step(greens[layer_at], lessers[layer_at], bonds[layer_at], right_green, right_lesser)
            density_rows[layer_at] = weighted_sum(weights, right_lesser)
            current_rows[layer_at] = weighted_sum(weights, current)
        return (carry[0] + jnp.stack(density_rows), carry[1] + jnp.stack(current_rows)), None

    zeros = jnp.zeros((layers, 2, onsite.shape[1], onsite.shape[1]), energies.dtype)
    totals = lax.scan(accumulate, (zeros, zeros), jnp.arange(NE, dtype=jnp.int32))[0]
    return totals[0], totals[1]
```

```python
import jax
import jax.numpy as jnp
from jax import lax
from jax.experimental import pallas as pl
from jax.experimental.pallas import tpu as pltpu
from jax.sharding import PartitionSpec as P

bf16 = jnp.bfloat16
f32 = jnp.float32
B = 256


def dot(a, b, tb=False):
    return lax.dot_general(
        a, b, (((1,), (1 if tb else 0,)), ((), ())), preferred_element_type=f32
    )


def split(x):
    high = x.astype(bf16)
    return high, (x - high.astype(f32)).astype(bf16)


def dot3(left, right, tb=False):
    return (
        dot(left[0], right[0], tb) + dot(left[0], right[1], tb) + dot(left[1], right[0], tb)
    )


def put(pair, at, x):
    high, low = split(x)
    pair[0][at] = high
    pair[1][at] = low


def put_left(pair, lead, row, re, im, conj):
    for ref, r, i in zip(pair, split(re), split(im)):
        top = lead + (pl.ds(row, B),)
        low = lead + (pl.ds(row + B, B),)
        a, b = pl.ds(0, B), pl.ds(B, B)
        ref[top + (a,)] = r
        ref[low + (a,)] = i
        ref[top + (b,)] = i if conj else -i
        ref[low + (b,)] = -r if conj else r


def sweeps(
    e_ref, k_ref, el_ref, ml_ref, et_ref, mt_ref, fermi_ref, bk_ref,
    onsite, broad, kdiag, couplings, density, current,
    gw_h, gw_l, pr_h, pr_l, x_h, x_l, s_h, s_l, a_h, a_l, v_h, v_l, vt_h, vt_l, gf, wf,
    blocks, from_core, to_plane, from_plane, to_line, from_line, to_owner, at_owner, owned,
    core_sems, plane_sems, line_sems, owner_sems,
):
    layers = onsite.shape[0] - 1
    gw, pr, xs, ss, aa, vv, vt = (
        (gw_h, gw_l), (pr_h, pr_l), (x_h, x_l), (s_h, s_l), (a_h, a_l), (v_h, v_l), (vt_h, vt_l)
    )
    energy = e_ref[0]
    moment = k_ref[0]
    weight = et_ref[el_ref[0]] * mt_ref[ml_ref[0]] * (1.0 / 256)
    me_e, me_k, me_l = lax.axis_index("energy"), lax.axis_index("kpt"), lax.axis_index("layer")
    me_x, me_z, me_c = lax.div(me_e, 4), lax.rem(lax.div(me_e, 2), 2), lax.rem(me_e, 2)

    def device(x, z, c, k, y):
        return ((x * 2 + z) * 2 + c, k, y)

    def core_peer():
        return device(me_x, me_z, 1 - me_c, me_k, me_l)

    def plane_peer(step):
        return lax.rem(me_x + step // 4, 4), lax.rem(me_l + step % 4, 4)

    def line_peer(step):
        return lax.rem(me_z + step // 4, 2), lax.rem(me_k + step % 4, 4)

    def owner_peer(step):
        return lax.rem(me_k + step // 4, 4), lax.rem(me_l + step % 4, 4)

    def plane_device(step):
        x, y = plane_peer(step)
        return device(x, me_z, me_c, me_k, y)

    def line_device(step):
        z, k = line_peer(step)
        return device(me_x, z, me_c, k, me_l)

    def owner_device(step):
        k, y = owner_peer(step)
        return device(me_x, me_z, me_c, k, y)

    barrier = pltpu.get_barrier_semaphore()
    peers = [core_peer()] + [plane_device(s) for s in range(1, 16)]
    peers += [line_device(s) for s in range(1, 8)] + [owner_device(s) for s in range(1, 16)]
    for peer in peers:
        pl.semaphore_signal(barrier, inc=1, device_id=peer, device_id_type=pl.DeviceIdType.MESH)

    def send(src, dst, sems, peer):
        pltpu.make_async_remote_copy(
            src_ref=src, dst_ref=dst, send_sem=sems[0], recv_sem=sems[1],
            device_id=peer, device_id_type=pl.DeviceIdType.MESH,
        ).start()

    def wait(like, sem):
        pltpu.make_async_copy(like, like, sem).wait()

    def core_start(i):
        send(blocks.at[i, :, :, :, 1 - me_c], from_core.at[i],
             (core_sems.at[0, i], core_sems.at[1, i]), core_peer())

    def core_finish(i):
        wait(from_core.at[i], core_sems.at[1, i])
        to_plane[i] = blocks[i, :, :, :, me_c] + from_core[i]

    def plane_start(i):
        for step in range(1, 16):
            x, y = plane_peer(step)
            send(to_plane.at[i, y, x], from_plane.at[i, step - 1],
                 (plane_sems.at[0, i], plane_sems.at[1, i]), plane_device(step))

    def plane_finish(i):
        wait(from_plane.at[i], plane_sems.at[1, i])
        total = to_plane[i, me_l, me_x]
        for step in range(1, 16):
            total = total + from_plane[i, step - 1]
        for z in range(2):
            for k in range(4):
                row, col = 8 * (k // 2), 128 * (k % 2)
                to_line[i, z, k] = total[z, row : row + 8, col : col + 128]

    def line_start(i):
        for step in range(1, 8):
            z, k = line_peer(step)
            send(to_line.at[i, z, k], from_line.at[i, step - 1],
                 (line_sems.at[0, i], line_sems.at[1, i]), line_device(step))

    def line_finish(i):
        wait(from_line.at[i], line_sems.at[1, i])
        total = to_line[i, me_z, me_k]
        for step in range(1, 8):
            total = total + from_line[i, step - 1]
        to_owner[i] = total

    def owner_exchange():
        for step in range(1, 16):
            k, y = owner_peer(step)
            send(to_owner.at[y], at_owner.at[step - 1],
                 (owner_sems.at[0], owner_sems.at[1]), owner_device(step))
        wait(at_owner, owner_sems.at[1])
        owned[me_l, me_k] = to_owner[me_l]
        for step in range(1, 16):
            k = lax.rem(me_k + 4 - step // 4, 4)
            y = lax.rem(me_l + 4 - step % 4, 4)
            owned[y, k] = at_owner[step - 1]
        for m in range(2):
            for k in range(4):
                at = (0, m, pl.ds(8 * (k // 2), 8), pl.ds(128 * (k % 2), 128))
                density[at] = owned[m, k]
                current[at] = owned[2 + m, k]

    eye = lax.broadcasted_iota(jnp.int32, (B, B), 0) == lax.broadcasted_iota(jnp.int32, (B, B), 1)
    get = lambda pair, *at: (pair[0][at], pair[1][at])

    def forward(i, inner):
        br = broad[i]
        gamma = br * jax.nn.sigmoid(jnp.full((1, B), (fermi_ref[i] - energy) / 0.25, f32))
        if inner:
            kind = bk_ref[i - 1]
            v = jnp.where(kind == 0, couplings[0], jnp.where(kind == 1, couplings[1], couplings[2]))
            put(vv, (slice(None),), v)
            put(vt, (slice(None),), v.T)
            p = dot3(get(gw), get(vv))
            put_left(pr, (i - 1,), 0, p[0:B], p[B : 2 * B], False)
            put_left(pr, (i - 1,), 2 * B, p[2 * B : 3 * B], p[3 * B :], True)
            left = get(vt)
            part = lambda j: dot3(left, get(pr, i - 1, pl.ds(j * B, B), pl.ds(0, B)))
            m_re = -onsite[i] - part(0)
            m_im = -part(1)
            s_re = part(2) + jnp.where(eye, gamma, 0.0)
            s_im = part(3)
        else:
            m_re = -onsite[i]
            s_re = jnp.where(eye, gamma, 0.0)
        shift = energy - moment * kdiag[i]
        dr = jnp.where(eye, m_re + shift, 0.0)
        dr_row, dr_col = jnp.sum(dr, 0, keepdims=True), jnp.sum(dr, 1, keepdims=True)
        half = 0.5 * br
        di = jnp.where(eye, (m_im + half) if inner else half, 0.0)
        di_row, di_col = jnp.sum(di, 0, keepdims=True), jnp.sum(di, 1, keepdims=True)
        n_row = 1.0 / (dr_row * dr_row + di_row * di_row)
        n_col = 1.0 / (dr_col * dr_col + di_col * di_col)
        rr, ri = dr_row * n_row, -di_row * n_row
        cr, ci = dr_col * n_col, -di_col * n_col
        off = jnp.where(eye, 0.0, m_re)
        if inner:
            off_im = jnp.where(eye, 0.0, m_im)
            a_re = cr * off - ci * off_im
            a_im = cr * off_im + ci * off
        else:
            a_re, a_im = cr * off, ci * off
        put_left(xs, (), 0, a_re, a_im, False)
        sq = dot3(get(xs, pl.ds(0, 2 * B), slice(None)), get(xs, pl.ds(0, 2 * B), pl.ds(0, B)))
        u_re, u_im = sq[0:B], sq[B:]
        put_left(aa, (), 0, u_re, u_im, False)
        cube = dot3(get(aa), get(xs, pl.ds(0, 2 * B), pl.ds(0, B)))
        t_re = jnp.where(eye, 1.0, 0.0) - a_re + (u_re - cube[0:B])
        t_im = (u_im - cube[B:]) - a_im
        g_re = t_re * rr - t_im * ri
        g_im = t_re * ri + t_im * rr
        gf[i, pl.ds(0, B)] = g_re
        gf[i, pl.ds(B, B)] = g_im
        put(gw, (pl.ds(0, B),), g_re)
        put(gw, (pl.ds(B, B),), g_im)
        if inner:
            put_left(aa, (), 0, g_re, g_im, False)
            put(ss, (pl.ds(0, B),), s_re)
            put(ss, (pl.ds(B, B),), s_im)
            t = dot3(get(aa), get(ss))
            t_re, t_im = t[0:B], t[B:]
        else:
            t_re, t_im = g_re * gamma, g_im * gamma
        put_left(xs, (), 0, t_re, t_im, True)
        w = dot3(get(xs, pl.ds(0, 2 * B), slice(None)), get(gw, pl.ds(0, 2 * B)))
        wf[i] = w
        put(gw, (pl.ds(2 * B, 2 * B),), w)

    forward(0, False)

    def forward_step(i, carry):
        forward(i, True)
        return carry

    lax.fori_loop(1, layers + 1, forward_step, 0)
    pl.semaphore_wait(barrier, len(peers))

    def report(i, m, x):
        blocks[i, m] = (weight * x).reshape(blocks.shape[2:])

    def reach(i, pw, zh, row):
        cur = pw + zh
        report(i, 2, cur[0:B])
        report(i, 3, cur[B:])
        mid = 0.5 * pw + zh
        put_left(xs, (), row, mid[0:B], mid[B:], False)

    def lesser(i, spread):
        h_re, h_im = spread[0:B], spread[B:]
        w_re = wf[i, pl.ds(0, B)] + (h_re + h_re.T)
        w_im = wf[i, pl.ds(B, B)] + (h_im - h_im.T)
        report(i, 0, w_re)
        report(i, 1, w_im)
        return w_re, w_im

    def backward_step(step, carry):
        i = layers - 1 - step
        qz = dot3(get(pr, i), get(gw, pl.ds(0, 2 * B)))
        pw = dot3(get(pr, i, pl.ds(0, 2 * B)), get(gw, pl.ds(2 * B, 2 * B)))
        put_left(xs, (), 0, qz[0:B], qz[B : 2 * B], True)
        reach(i, pw, qz[2 * B :], 2 * B)

        @pl.when(step >= 1)
        def _():
            core_finish(i + 1)
            plane_start(i + 1)

        spread = dot3(get(xs), get(pr, i, pl.ds(0, B)), True)
        put(gw, (pl.ds(0, 2 * B),), gf[i] + spread[0 : 2 * B])
        w_re, w_im = lesser(i, spread[2 * B :])
        put(gw, (pl.ds(2 * B, B),), w_re)
        put(gw, (pl.ds(3 * B, B),), w_im)

        core_start(i)

        @pl.when(step >= 2)
        def _():
            plane_finish(i + 2)
            line_start(i + 2)

        return carry

    lax.fori_loop(0, layers - 1, backward_step, 0)
    zh = dot3(get(pr, 0, pl.ds(2 * B, 2 * B)), get(gw, pl.ds(0, 2 * B)))
    pw = dot3(get(pr, 0, pl.ds(0, 2 * B)), get(gw, pl.ds(2 * B, 2 * B)))
    reach(0, pw, zh, 0)
    core_finish(1)
    plane_start(1)
    spread = dot3(get(xs, pl.ds(0, 2 * B)), get(pr, 0, pl.ds(0, B)), True)
    lesser(0, spread)
    core_start(0)
    plane_finish(2)
    line_start(2)
    core_finish(0)
    plane_start(0)
    plane_finish(1)
    line_start(1)
    plane_finish(0)
    line_start(0)
    for i in (3, 2, 1, 0):
        line_finish(i)
    owner_exchange()
    for i in range(layers):
        wait(from_core.at[i], core_sems.at[0, i])
        wait(from_plane.at[i], plane_sems.at[0, i])
        wait(from_line.at[i], line_sems.at[0, i])
    wait(at_owner, owner_sems.at[0])


def scratch(layers):
    pair = lambda *s: [pltpu.VMEM(s, bf16), pltpu.VMEM(s, bf16)]
    full = lambda *s: pltpu.VMEM(s, f32)
    return (
        pair(4 * B, B) + pair(layers, 4 * B, 2 * B) + pair(4 * B, 2 * B) + pair(2 * B, B)
        + pair(2 * B, 2 * B) + pair(B, B) + pair(B, B)
        + [full(layers + 1, 2 * B, B)] * 2
        + [
            full(layers, 4, 4, 2, 2, 16, B),
            full(layers, 4, 4, 2, 16, B),
            full(layers, 4, 4, 2, 16, B),
            full(layers, 15, 2, 16, B),
            full(layers, 2, 4, 8, 128),
            full(layers, 7, 8, 128),
            full(layers, 8, 128),
            full(15, 8, 128),
            full(4, 4, 8, 128),
            pltpu.SemaphoreType.DMA((2, layers)),
            pltpu.SemaphoreType.DMA((2, layers)),
            pltpu.SemaphoreType.DMA((2, layers)),
            pltpu.SemaphoreType.DMA((2,)),
        ]
    )


def per_device(
    energies, momenta, energy_level, momentum_level, energy_table, momentum_table,
    onsite, broad, kdiag, fermi, couplings, bond_kind,
):
    smem = pl.BlockSpec(memory_space=pltpu.SMEM)
    vmem = pl.BlockSpec(memory_space=pltpu.VMEM)
    layers = onsite.shape[0] - 1
    result = jax.ShapeDtypeStruct((1, 2, 16, B), f32)
    return pl.pallas_call(
        sweeps,
        out_shape=(result, result),
        in_specs=[smem] * 8 + [vmem] * 4,
        out_specs=(vmem, vmem),
        scratch_shapes=scratch(layers),
        compiler_params=pltpu.CompilerParams(
            vmem_limit_bytes=62 << 20, collective_id=0, has_side_effects=True
        ),
        name="sweeps",
    )(
        energies, momenta, energy_level, momentum_level, energy_table, momentum_table,
        fermi, bond_kind, onsite, broad[:, None, :], kdiag[:, None, :], couplings,
    )


def solution(mesh):
    rep = P()
    both = P(("energy", "layer"))
    return jax.shard_map(
        per_device,
        mesh=mesh,
        in_specs=(both, P("kpt"), both, P("kpt"), rep, rep, rep, rep, rep, rep, rep, rep),
        out_specs=(P("layer", None, "energy", None), P("layer", None, "energy", None)),
        check_vma=False,
    )
```

```python
import jax
import jax.numpy as jnp
from jax import lax
from jax.experimental import pallas as pl
from jax.experimental.pallas import tpu as pltpu
from jax.sharding import PartitionSpec as P

bf16 = jnp.bfloat16
f32 = jnp.float32
B = 256
CH = 32


def dot(a, b, tb=False):
    return lax.dot_general(
        a, b, (((1,), (1 if tb else 0,)), ((), ())), preferred_element_type=f32
    )


def split(x):
    high = x.astype(bf16)
    return high, (x - high.astype(f32)).astype(bf16)


def dot3(left, right, tb=False):
    return (
        dot(left[0], right[0], tb) + dot(left[0], right[1], tb) + dot(left[1], right[0], tb)
    )


def get(pair, *at):
    return pair[0][at], pair[1][at]


def put(pair, at, x):
    pair[0][at], pair[1][at] = split(x)


def put_left(pair, lead, row, rows, re, im, conj):
    for ref, r, i in zip(pair, split(re), split(im)):
        top, low = lead + (pl.ds(row, rows),), lead + (pl.ds(row + B, rows),)
        a, b = pl.ds(0, B), pl.ds(B, B)
        ref[top + (a,)] = r
        ref[low + (a,)] = i
        ref[top + (b,)] = i if conj else -i
        ref[low + (b,)] = -r if conj else r


def chunks():
    for r in range(0, B, CH):
        yield r, slice(r, r + CH), slice(B + r, B + r + CH)


def sweeps(
    *refs,
):
    scalars, inputs, result = refs[:8], refs[8:12], refs[12]
    held, in_sems, rest = refs[13:17], refs[17], refs[18:]
    copies = [pltpu.make_async_copy(a, b, in_sems.at[n]) for n, (a, b) in enumerate(zip(inputs, held))]
    for copy in copies:
        copy.start()
    sweep_body(copies, result, *scalars, *held, *rest)


def sweep_body(
    copies, result, e_ref, k_ref, el_ref, ml_ref, et_ref, mt_ref, fermi_ref, bk_ref,
    broad, kdiag, couplings, onsite,
    gs_h, gs_l, gl_h, gl_l, ws_h, ws_l, pr_h, pr_l, al_h, al_l, ul_h, ul_l, ss_h, ss_l,
    tl_h, tl_l, ml_h, ml_l, v_h, v_l, vt_h, vt_l, gf, wf, mf, hf,
    blocks, from_core, to_plane, from_first, to_second, from_second, to_line, from_line, to_owner, at_owner, owned,
    core_sems, first_sems, second_sems, line_sems, owner_sems,
):
    layers = onsite.shape[0] - 1
    gs, gl, ws, pr, al, ul, ss, tl, ml, vv, vt = (
        (gs_h, gs_l), (gl_h, gl_l), (ws_h, ws_l), (pr_h, pr_l), (al_h, al_l), (ul_h, ul_l),
        (ss_h, ss_l), (tl_h, tl_l), (ml_h, ml_l), (v_h, v_l), (vt_h, vt_l),
    )
    for copy in copies:
        copy.wait()
    energy = e_ref[0]
    moment = k_ref[0]
    weight = et_ref[el_ref[0]] * mt_ref[ml_ref[0]] * (1.0 / 256)
    me_e, me_k, me_l = lax.axis_index("energy"), lax.axis_index("kpt"), lax.axis_index("layer")
    me_x, me_z, me_c = lax.div(me_e, 4), lax.rem(lax.div(me_e, 2), 2), lax.rem(me_e, 2)

    def device(x, z, c, k, y):
        return ((x * 2 + z) * 2 + c, k, y)

    def core_peer():
        return device(me_x, me_z, 1 - me_c, me_k, me_l)

    def after(at, step):
        return lax.rem(at + step, 4)

    def x_device(step):
        return device(after(me_x, step), me_z, me_c, me_k, me_l)

    def y_device(step):
        return device(me_x, me_z, me_c, me_k, after(me_l, step))

    def line_peer(step):
        return lax.rem(me_z + step // 4, 2), lax.rem(me_k + step % 4, 4)

    def owner_peer(step):
        return lax.rem(me_k + step // 4, 4), lax.rem(me_l + step % 4, 4)

    def line_device(step):
        z, k = line_peer(step)
        return device(me_x, z, me_c, k, me_l)

    def owner_device(step):
        k, y = owner_peer(step)
        return device(me_x, me_z, me_c, k, y)

    barrier = pltpu.get_barrier_semaphore()
    peers = [core_peer()] + [x_device(s) for s in range(1, 4)]
    peers += [line_device(s) for s in range(1, 8)] + [owner_device(s) for s in range(1, 16)]
    for peer in peers:
        pl.semaphore_signal(barrier, inc=1, device_id=peer, device_id_type=pl.DeviceIdType.MESH)

    def send(src, dst, sems, peer):
        pltpu.make_async_remote_copy(
            src_ref=src, dst_ref=dst, send_sem=sems[0], recv_sem=sems[1],
            device_id=peer, device_id_type=pl.DeviceIdType.MESH,
        ).start()

    def wait(like, sem):
        pltpu.make_async_copy(like, like, sem).wait()

    def core_start(i):
        send(blocks.at[i, :, :, :, 1 - me_c], from_core.at[i],
             (core_sems.at[0, i], core_sems.at[1, i]), core_peer())

    def core_finish(i):
        wait(from_core.at[i], core_sems.at[1, i])
        to_plane[i] = blocks[i, :, :, :, me_c] + from_core[i]

    def plane_start(i):
        for step in range(1, 4):
            send(to_plane.at[i, :, after(me_x, step), 0], from_first.at[i, 0, step - 1],
                 (first_sems.at[0, 0, i], first_sems.at[1, 0, i]), x_device(step))
            send(to_plane.at[i, after(me_l, step), :, 1], from_first.at[i, 1, step - 1],
                 (first_sems.at[0, 1, i], first_sems.at[1, 1, i]), y_device(step))

    def plane_turn(i):
        for way in range(2):
            wait(from_first.at[i, way], first_sems.at[1, way, i])
            own = to_plane[i, :, me_x, 0] if way == 0 else to_plane[i, me_l, :, 1]
            to_second[i, way] = own + from_first[i, way, 0] + (
                from_first[i, way, 1] + from_first[i, way, 2]
            )
        for step in range(1, 4):
            send(to_second.at[i, 0, after(me_l, step)], from_second.at[i, 0, step - 1],
                 (second_sems.at[0, 0, i], second_sems.at[1, 0, i]), y_device(step))
            send(to_second.at[i, 1, after(me_x, step)], from_second.at[i, 1, step - 1],
                 (second_sems.at[0, 1, i], second_sems.at[1, 1, i]), x_device(step))

    def plane_finish(i):
        for z in range(2):
            wait(from_second.at[i, z], second_sems.at[1, z, i])
            total = to_second[i, z, me_l if z == 0 else me_x] + from_second[i, z, 0] + (
                from_second[i, z, 1] + from_second[i, z, 2]
            )
            for k in range(4):
                row, col = 8 * (k // 2), 128 * (k % 2)
                to_line[i, z, k] = total[row : row + 8, col : col + 128]

    def line_start(i):
        for step in range(1, 8):
            z, k = line_peer(step)
            send(to_line.at[i, z, k], from_line.at[i, step - 1],
                 (line_sems.at[0, i], line_sems.at[1, i]), line_device(step))

    def line_finish(i):
        wait(from_line.at[i], line_sems.at[1, i])
        total = to_line[i, me_z, me_k]
        for step in range(1, 8):
            total = total + from_line[i, step - 1]
        to_owner[i] = total

    def owner_exchange():
        for step in range(1, 16):
            k, y = owner_peer(step)
            send(to_owner.at[y], at_owner.at[step - 1],
                 (owner_sems.at[0], owner_sems.at[1]), owner_device(step))
        wait(at_owner, owner_sems.at[1])
        owned[me_l, me_k] = to_owner[me_l]
        for step in range(1, 16):
            k = lax.rem(me_k + 4 - step // 4, 4)
            y = lax.rem(me_l + 4 - step % 4, 4)
            owned[y, k] = at_owner[step - 1]
        for m in range(4):
            for k in range(4):
                result[m, pl.ds(8 * (k // 2), 8), pl.ds(128 * (k % 2), 128)] = owned[m, k]

    both, first = pl.ds(0, 2 * B), pl.ds(0, B)

    def diagonal_of(r, lanes):
        at = r % 128 if lanes == 128 else r
        return (
            lax.broadcasted_iota(jnp.int32, (CH, lanes), 0) + at
            == lax.broadcasted_iota(jnp.int32, (CH, lanes), 1)
        )

    def source(i):
        br = broad[pl.ds(i, 1), :]
        return br * jax.nn.sigmoid(jnp.full((1, B), (fermi_ref[i] - energy) / 0.25, f32))

    def inverse_ends(i):
        shift = energy - moment * kdiag[pl.ds(i, 1), :]
        half = 0.5 * broad[pl.ds(i, 1), :]
        rows = []
        cols = {}
        for t in range(2):
            lane = slice(128 * t, 128 * t + 128)
            dr_row = di_row = 0.0
            for r in range(128 * t, 128 * t + 128, CH):
                on = diagonal_of(r, 128)
                dr = jnp.where(on, mf[0, pl.ds(r, CH), lane] + shift[:, lane], 0.0)
                di = jnp.where(on, mf[1, pl.ds(r, CH), lane] + half[:, lane], 0.0)
                dr_row = dr_row + jnp.sum(dr, 0, keepdims=True)
                di_row = di_row + jnp.sum(di, 0, keepdims=True)
                a, b = jnp.sum(dr, 1, keepdims=True), jnp.sum(di, 1, keepdims=True)
                n = 1.0 / (a * a + b * b)
                cols[r] = (a * n, -b * n)
            n = 1.0 / (dr_row * dr_row + di_row * di_row)
            rows.append((dr_row * n, -di_row * n))
        return tuple(jnp.concatenate([rows[0][c], rows[1][c]], 1) for c in range(2)), cols

    def green_from(i, between):
        (rr, ri), cols = inverse_ends(i)
        for r, _, _ in chunks():
            on = diagonal_of(r, B)
            m_re = jnp.where(on, 0.0, mf[0, pl.ds(r, CH)])
            m_im = jnp.where(on, 0.0, mf[1, pl.ds(r, CH)])
            cr, ci = cols[r]
            a_re = cr * m_re - ci * m_im
            a_im = cr * m_im + ci * m_re
            put_left(al, (), r, CH, a_re, a_im, False)
            mf[0, pl.ds(r, CH)] = jnp.where(on, 1.0, 0.0) - a_re
            mf[1, pl.ds(r, CH)] = -a_im
        sq = dot3(get(al), get(al, both, first))
        between(0)
        for r, a, b in chunks():
            u_re, u_im = sq[a], sq[b]
            put_left(ul, (), r, CH, u_re, u_im, False)
            mf[0, pl.ds(r, CH)] += u_re
            mf[1, pl.ds(r, CH)] += u_im
        cube = dot3(get(ul), get(al, both, first))
        between(1)
        for r, a, b in chunks():
            t_re = mf[0, pl.ds(r, CH)] - cube[a]
            t_im = mf[1, pl.ds(r, CH)] - cube[b]
            g_re = t_re * rr - t_im * ri
            g_im = t_re * ri + t_im * rr
            gf[i, pl.ds(r, CH)] = g_re
            gf[i, pl.ds(B + r, CH)] = g_im
            put(gs, (pl.ds(r, CH),), g_re)
            put(gs, (pl.ds(B + r, CH),), g_im)
            put_left(gl, (), r, CH, g_re, g_im, False)

    def put_source(i, s_re, s_im):
        gamma = source(i)
        for r, a, _ in chunks():
            x = jnp.where(diagonal_of(r, B), gamma, 0.0)
            if s_re is not None:
                x = x + s_re[a]
            put(ss, (pl.ds(r, CH),), x)
            put(ss, (pl.ds(B + r, CH),), jnp.zeros((CH, B), f32) if s_im is None else s_im[a])

    def lesser_left():
        t = dot3(get(gl), get(ss))
        for r, a, b in chunks():
            put_left(tl, (), r, CH, t[a], t[b], True)

    def lesser_of(i):
        w = dot3(get(tl), get(gs))
        for r, a, b in chunks():
            for at, x in ((r, w[a]), (B + r, w[b])):
                wf[i, pl.ds(at, CH)] = x
                put(ws, (pl.ds(at, CH),), x)

    for r, _, _ in chunks():
        mf[0, pl.ds(r, CH)] = -onsite[0, pl.ds(r, CH)]
        mf[1, pl.ds(r, CH)] = jnp.zeros((CH, B), f32)
    put_source(0, None, None)
    green_from(0, lambda stage: None)

    def forward_step(i, carry):
        kind = bk_ref[i - 1]
        v = jnp.where(kind == 0, couplings[0], jnp.where(kind == 1, couplings[1], couplings[2]))
        put(vv, (slice(None),), v)
        put(vt, (slice(None),), v.T)
        p = dot3(get(gs), get(vv))
        for r, a, b in chunks():
            put_left(pr, (i - 1,), r, CH, p[a], p[b], False)
        lesser_left()
        part = lambda j: dot3(get(vt), get(pr, i - 1, pl.ds(j * B, B), first))
        m = part(0), part(1)
        for r, a, _ in chunks():
            mf[0, pl.ds(r, CH)] = -onsite[i, pl.ds(r, CH)] - m[0][a]
            mf[1, pl.ds(r, CH)] = -m[1][a]
        lesser_of(i - 1)

        def between(stage):
            if stage == 0:
                q = dot3(get(ws), get(vv))
                for r, a, b in chunks():
                    put_left(pr, (i - 1,), 2 * B + r, CH, q[a], q[b], True)
            else:
                put_source(i, part(2), part(3))

        green_from(i, between)
        return carry

    lax.fori_loop(1, layers + 1, forward_step, 0)
    pl.semaphore_wait(barrier, len(peers))
    lesser_left()
    lesser_of(layers)
    hf[...] = jnp.zeros_like(hf)

    def report(i, m, r, x):
        if i == layers:
            return
        x = weight * x
        for half in range(0, CH, 16):
            e = (r + half) // 16
            blocks[i, m, e // 4, e // 2 % 2, e % 2] = x[half : half + 16]

    def finish(i, last):
        h_re, h_im = hf[0].T, hf[1].T
        for r, a, _ in chunks():
            w_re = wf[i, pl.ds(r, CH)] + (hf[0, pl.ds(r, CH)] + h_re[a])
            w_im = wf[i, pl.ds(B + r, CH)] + (hf[1, pl.ds(r, CH)] - h_im[a])
            report(i, 0, r, w_re)
            report(i, 1, r, w_im)
            if not last:
                put(ws, (pl.ds(r, CH),), w_re)
                put(ws, (pl.ds(B + r, CH),), w_im)

    def backward(i, inner):
        ends = get(pr, i, first)
        if inner:
            qz = dot3(get(pr, i), get(gs))
            zh = qz[2 * B :]
        else:
            zh = dot3(get(pr, i, pl.ds(2 * B, 2 * B)), get(gs))
        finish(i + 1, False)
        if i < layers - 1:
            core_start(i + 1)
        pw = dot3(get(pr, i, both), get(ws))
        if inner:
            for r, a, b in chunks():
                put_left(al, (), r, CH, qz[a], qz[b], True)
            grown = dot3(get(al), ends, True)
        for r, a, b in chunks():
            cur = pw[a] + zh[a], pw[b] + zh[b]
            report(i, 2, r, cur[0])
            report(i, 3, r, cur[1])
            put_left(ml, (), r, CH, cur[0] - 0.5 * pw[a], cur[1] - 0.5 * pw[b], False)
        if inner:
            for r, a, b in chunks():
                put(gs, (pl.ds(r, CH),), gf[i, pl.ds(r, CH)] + grown[a])
                put(gs, (pl.ds(B + r, CH),), gf[i, pl.ds(B + r, CH)] + grown[b])
        h = dot3(get(ml), ends, True)
        hf[0] = h[0:B]
        hf[1] = h[B:]
        if i == 0:
            plane_turn(3)
        if i < layers - 1:
            core_finish(i + 1)
            plane_start(i + 1)

    backward(3, True)
    for i in (2, 1, 0):
        backward(i, i > 0)
    finish(0, True)
    core_start(0)
    plane_turn(2)
    core_finish(0)
    plane_start(0)
    plane_finish(3)
    line_start(3)
    plane_turn(1)
    plane_finish(2)
    line_start(2)
    plane_turn(0)
    plane_finish(1)
    line_start(1)
    for i in (3, 2, 1):
        line_finish(i)
    plane_finish(0)
    line_start(0)
    line_finish(0)
    owner_exchange()
    for i in range(layers):
        wait(from_core.at[i], core_sems.at[0, i])
        for way in range(2):
            wait(from_first.at[i, way], first_sems.at[0, way, i])
            wait(from_second.at[i, way], second_sems.at[0, way, i])
        wait(from_line.at[i], line_sems.at[0, i])
    wait(at_owner, owner_sems.at[0])


def scratch(layers):
    pair = lambda *s: [pltpu.VMEM(s, bf16), pltpu.VMEM(s, bf16)]
    full = lambda *s: pltpu.VMEM(s, f32)
    wide = pair(2 * B, 2 * B)
    return (
        pair(2 * B, B) + wide + pair(2 * B, B) + pair(layers, 4 * B, 2 * B) + wide + wide
        + pair(2 * B, B) + wide + wide + pair(B, B) + pair(B, B)
        + [full(layers + 1, 2 * B, B)] * 2 + [full(2, B, B)] * 2
        + [
            full(layers, 4, 4, 2, 2, 16, B),
            full(layers, 4, 4, 2, 16, B),
            full(layers, 4, 4, 2, 16, B),
            full(layers, 2, 3, 4, 16, B),
            full(layers, 2, 4, 16, B),
            full(layers, 2, 3, 16, B),
            full(layers, 2, 4, 8, 128),
            full(layers, 7, 8, 128),
            full(layers, 8, 128),
            full(15, 8, 128),
            full(4, 4, 8, 128),
            pltpu.SemaphoreType.DMA((2, layers)),
            pltpu.SemaphoreType.DMA((2, 2, layers)),
            pltpu.SemaphoreType.DMA((2, 2, layers)),
            pltpu.SemaphoreType.DMA((2, layers)),
            pltpu.SemaphoreType.DMA((2,)),
        ]
    )


def per_device(
    energies, momenta, energy_level, momentum_level, energy_table, momentum_table,
    onsite, broad, kdiag, fermi, couplings, bond_kind,
):
    layers = onsite.shape[0] - 1
    args = (
        energies, momenta, energy_level, momentum_level, energy_table, momentum_table,
        fermi, bond_kind, broad, kdiag, couplings, onsite,
    )
    held = [pltpu.VMEM(x.shape, x.dtype) for x in args[8:]]
    owned = pl.pallas_call(
        sweeps,
        out_shape=jax.ShapeDtypeStruct((4, 16, B), f32),
        in_specs=[pl.BlockSpec(memory_space=pltpu.SMEM)] * 8 + [pl.BlockSpec(memory_space=pl.ANY)] * 4,
        out_specs=pl.BlockSpec(memory_space=pltpu.VMEM),
        scratch_shapes=held + [pltpu.SemaphoreType.DMA((4,))] + scratch(layers),
        compiler_params=pltpu.CompilerParams(
            vmem_limit_bytes=62 << 20, collective_id=0, has_side_effects=True
        ),
        name="sweeps",
    )(*args)
    return owned[None, :2], owned[None, 2:]


def solution(mesh):
    rep = P()
    both = P(("energy", "layer"))
    return jax.shard_map(
        per_device,
        mesh=mesh,
        in_specs=(both, P("kpt"), both, P("kpt"), rep, rep, rep, rep, rep, rep, rep, rep),
        out_specs=(P("layer", None, "energy", None), P("layer", None, "energy", None)),
        check_vma=False,
    )
```

```python
import jax
import jax.numpy as jnp
from jax import lax
from jax.experimental import pallas as pl
from jax.experimental.pallas import tpu as pltpu
from jax.sharding import PartitionSpec as P

bf16 = jnp.bfloat16
f32 = jnp.float32
B = 256
CH = 32


def dot(a, b, tb=False):
    return lax.dot_general(
        a, b, (((1,), (1 if tb else 0,)), ((), ())), preferred_element_type=f32
    )


def split(x):
    high = x.astype(bf16)
    return high, (x - high.astype(f32)).astype(bf16)


def dot3(left, right, tb=False):
    return (
        dot(left[0], right[0], tb) + dot(left[0], right[1], tb) + dot(left[1], right[0], tb)
    )


def get(pair, *at):
    return pair[0][at], pair[1][at]


def put(pair, at, x):
    pair[0][at], pair[1][at] = split(x)


def put3(pair, lead, at, stride, re, im, conj):
    for n, x in enumerate((re, im, re - im if conj else re + im)):
        put(pair, lead + (pl.ds(at + n * stride, CH),), x)


def product(left, right, conj=False, tb=False):
    t1, t2, t3 = (dot3(left(n), right(n), tb) for n in range(3))

    def rows(a):
        if conj:
            return t1[a] + t2[a], (t1[a] - t2[a]) - t3[a]
        return t1[a] - t2[a], t3[a] - (t1[a] + t2[a])

    return rows


def thirds(pair, *lead):
    return lambda n: get(pair, *lead, pl.ds(n * B, B))


def chunks():
    for r in range(0, B, CH):
        yield r, slice(r, r + CH), slice(B + r, B + r + CH)


def sweeps(
    *refs,
):
    scalars, inputs, result = refs[:8], refs[8:12], refs[12]
    held, in_sems, rest = refs[13:17], refs[17], refs[18:]
    broad, kdiag, couplings, onsite = zip(inputs, held)
    first, rest_of = pl.ds(0, 1), pl.ds(1, onsite[0].shape[0] - 1)
    pairs = [broad, kdiag, [x.at[first] for x in onsite], couplings, [x.at[rest_of] for x in onsite]]
    copies = [pltpu.make_async_copy(a, b, in_sems.at[n]) for n, (a, b) in enumerate(pairs)]
    for copy in copies:
        copy.start()
    sweep_body(copies, result, *scalars, *held, *rest)


def sweep_body(
    copies, result, e_ref, k_ref, el_ref, ml_ref, et_ref, mt_ref, fermi_ref, bk_ref,
    broad, kdiag, couplings, onsite,
    gs_h, gs_l, ws_h, ws_l, pr_h, pr_l, al_h, al_l, ul_h, ul_l, ss_h, ss_l,
    tl_h, tl_l, ml_h, ml_l, v_h, v_l, vt_h, vt_l, gf, wf, mf, hf,
    blocks, from_core, to_plane, from_first, to_second, from_second, to_line, from_line, to_owner, many,
    core_sems, first_sems, second_sems, line_sems, owner_sems,
):
    layers = onsite.shape[0] - 1
    gs, ws, pr, al, ul, ss, tl, ml, vv, vt = (
        (gs_h, gs_l), (ws_h, ws_l), (pr_h, pr_l), (al_h, al_l), (ul_h, ul_l),
        (ss_h, ss_l), (tl_h, tl_l), (ml_h, ml_l), (v_h, v_l), (vt_h, vt_l),
    )
    energy = e_ref[0]
    moment = k_ref[0]
    weight = et_ref[el_ref[0]] * mt_ref[ml_ref[0]] * (1.0 / 256)
    me_e, me_k, me_l = lax.axis_index("energy"), lax.axis_index("kpt"), lax.axis_index("layer")
    me_x, me_z, me_c = lax.div(me_e, 4), lax.rem(lax.div(me_e, 2), 2), lax.rem(me_e, 2)

    def device(x, z, c, k, y):
        return ((x * 2 + z) * 2 + c, k, y)

    def core_peer():
        return device(me_x, me_z, 1 - me_c, me_k, me_l)

    def after(at, step):
        return lax.rem(at + step, 4)

    def x_device(step):
        return device(after(me_x, step), me_z, me_c, me_k, me_l)

    def y_device(step):
        return device(me_x, me_z, me_c, me_k, after(me_l, step))

    def line_peer(step):
        return lax.rem(me_z + step // 4, 2), lax.rem(me_k + step % 4, 4)

    def owner_peer(step):
        return lax.rem(me_k + step // 4, 4), lax.rem(me_l + step % 4, 4)

    def line_device(step):
        z, k = line_peer(step)
        return device(me_x, z, me_c, k, me_l)

    def owner_device(step):
        k, y = owner_peer(step)
        return device(me_x, me_z, me_c, k, y)

    barrier = pltpu.get_barrier_semaphore()
    peers = [core_peer()] + [x_device(s) for s in range(1, 4)]
    peers += [line_device(s) for s in range(1, 8)] + [owner_device(s) for s in range(1, 16)]
    for peer in peers:
        pl.semaphore_signal(barrier, inc=1, device_id=peer, device_id_type=pl.DeviceIdType.MESH)

    def send(src, dst, sems, peer):
        pltpu.make_async_remote_copy(
            src_ref=src, dst_ref=dst, send_sem=sems[0], recv_sem=sems[1],
            device_id=peer, device_id_type=pl.DeviceIdType.MESH,
        ).start()

    def wait(like, sem):
        pltpu.make_async_copy(like, like, sem).wait()

    def core_start(i):
        send(blocks.at[i, :, :, :, 1 - me_c], from_core.at[i],
             (core_sems.at[0, i], core_sems.at[1, i]), core_peer())

    def core_finish(i):
        wait(from_core.at[i], core_sems.at[1, i])
        to_plane[i] = blocks[i, :, :, :, me_c] + from_core[i]

    def plane_start(i):
        for step in range(1, 4):
            send(to_plane.at[i, :, after(me_x, step), 0], from_first.at[i, 0, step - 1],
                 (first_sems.at[0, 0, i], first_sems.at[1, 0, i]), x_device(step))
            send(to_plane.at[i, after(me_l, step), :, 1], from_first.at[i, 1, step - 1],
                 (first_sems.at[0, 1, i], first_sems.at[1, 1, i]), y_device(step))

    def plane_turn(i):
        for way in range(2):
            wait(from_first.at[i, way], first_sems.at[1, way, i])
            own = to_plane[i, :, me_x, 0] if way == 0 else to_plane[i, me_l, :, 1]
            to_second[i, way] = own + from_first[i, way, 0] + (
                from_first[i, way, 1] + from_first[i, way, 2]
            )
        for step in range(1, 4):
            send(to_second.at[i, 0, after(me_l, step)], from_second.at[i, 0, step - 1],
                 (second_sems.at[0, 0, i], second_sems.at[1, 0, i]), y_device(step))
            send(to_second.at[i, 1, after(me_x, step)], from_second.at[i, 1, step - 1],
                 (second_sems.at[0, 1, i], second_sems.at[1, 1, i]), x_device(step))

    def plane_finish(i):
        for z in range(2):
            wait(from_second.at[i, z], second_sems.at[1, z, i])
            total = to_second[i, z, me_l if z == 0 else me_x] + from_second[i, z, 0] + (
                from_second[i, z, 1] + from_second[i, z, 2]
            )
            for k in range(4):
                row, col = 8 * (k // 2), 128 * (k % 2)
                to_line[i, z, k] = total[row : row + 8, col : col + 128]

    def line_start(i):
        for step in range(1, 8):
            z, k = line_peer(step)
            send(to_line.at[i, z, k], from_line.at[i, step - 1],
                 (line_sems.at[0, i], line_sems.at[1, i]), line_device(step))

    def line_finish(i):
        wait(from_line.at[i], line_sems.at[1, i])
        total = to_line[i, me_z, me_k]
        for step in range(1, 8):
            total = total + from_line[i, step - 1]
        to_owner[i] = total

    def owner_exchange():
        mine = result.at[me_l, lax.div(me_k, 2), :, pl.ds(pl.multiple_of(128 * lax.rem(me_k, 2), 128), 128)]
        for step in range(1, 16):
            k, y = owner_peer(step)
            send(to_owner.at[y], mine, (owner_sems.at[0], owner_sems.at[1]), owner_device(step))
        own = pltpu.make_async_copy(to_owner.at[me_l], mine, owner_sems.at[2])
        own.start()
        own.wait()
        wait(many, owner_sems.at[1])

    for copy in copies[:3]:
        copy.wait()
    both = pl.ds(0, 2 * B)

    def diagonal_of(r, lanes):
        at = r % 128 if lanes == 128 else r
        return (
            lax.broadcasted_iota(jnp.int32, (CH, lanes), 0) + at
            == lax.broadcasted_iota(jnp.int32, (CH, lanes), 1)
        )

    def source(i):
        br = broad[pl.ds(i, 1), :]
        return br * jax.nn.sigmoid(jnp.full((1, B), (fermi_ref[i] - energy) / 0.25, f32))

    def inverse_ends(i):
        shift = energy - moment * kdiag[pl.ds(i, 1), :]
        half = 0.5 * broad[pl.ds(i, 1), :]
        rows = []
        cols = {}
        for t in range(2):
            lane = slice(128 * t, 128 * t + 128)
            dr_row = di_row = 0.0
            for r in range(128 * t, 128 * t + 128, CH):
                on = diagonal_of(r, 128)
                dr = jnp.where(on, mf[0, pl.ds(r, CH), lane] + shift[:, lane], 0.0)
                di = jnp.where(on, mf[1, pl.ds(r, CH), lane] + half[:, lane], 0.0)
                dr_row = dr_row + jnp.sum(dr, 0, keepdims=True)
                di_row = di_row + jnp.sum(di, 0, keepdims=True)
                a, b = jnp.sum(dr, 1, keepdims=True), jnp.sum(di, 1, keepdims=True)
                n = 1.0 / (a * a + b * b)
                cols[r] = (a * n, -b * n)
            n = 1.0 / (dr_row * dr_row + di_row * di_row)
            rows.append((dr_row * n, -di_row * n))
        return tuple(jnp.concatenate([rows[0][c], rows[1][c]], 1) for c in range(2)), cols

    def green_from(i, between):
        (rr, ri), cols = inverse_ends(i)
        for r, _, _ in chunks():
            on = diagonal_of(r, B)
            m_re = jnp.where(on, 0.0, mf[0, pl.ds(r, CH)])
            m_im = jnp.where(on, 0.0, mf[1, pl.ds(r, CH)])
            cr, ci = cols[r]
            a_re = cr * m_re - ci * m_im
            a_im = cr * m_im + ci * m_re
            put3(al, (), r, B, a_re, a_im, False)
            mf[0, pl.ds(r, CH)] = jnp.where(on, 1.0, 0.0) - a_re
            mf[1, pl.ds(r, CH)] = -a_im
        sq = product(thirds(al), thirds(al))
        between(0)
        for r, a, _ in chunks():
            u_re, u_im = sq(a)
            put3(ul, (), r, B, u_re, u_im, False)
            mf[0, pl.ds(r, CH)] += u_re
            mf[1, pl.ds(r, CH)] += u_im
        cube = product(thirds(ul), thirds(al))
        between(1)
        for r, a, _ in chunks():
            c_re, c_im = cube(a)
            t_re = mf[0, pl.ds(r, CH)] - c_re
            t_im = mf[1, pl.ds(r, CH)] - c_im
            g_re = t_re * rr - t_im * ri
            g_im = t_re * ri + t_im * rr
            gf[i, pl.ds(r, CH)] = g_re
            gf[i, pl.ds(B + r, CH)] = g_im
            put3(gs, (), r, B, g_re, g_im, False)

    def put_source(i, s_re, s_im):
        gamma = source(i)
        for r, a, _ in chunks():
            x = jnp.where(diagonal_of(r, B), gamma, 0.0)
            if s_re is not None:
                x = x + s_re[a]
            put3(ss, (), r, B, x, jnp.zeros((CH, B), f32) if s_im is None else s_im[a], False)

    def lesser_left():
        t = product(thirds(gs), thirds(ss))
        for r, a, _ in chunks():
            put3(tl, (), r, B, *t(a), True)

    def lesser_of(i):
        w = product(thirds(tl), thirds(gs), True)
        for r, a, _ in chunks():
            w_re, w_im = w(a)
            wf[i, pl.ds(r, CH)] = w_re
            wf[i, pl.ds(B + r, CH)] = w_im
            put(ws, (pl.ds(r, CH),), w_re)
            put(ws, (pl.ds(B + r, CH),), w_im)

    for r, _, _ in chunks():
        mf[0, pl.ds(r, CH)] = -onsite[0, pl.ds(r, CH)]
        mf[1, pl.ds(r, CH)] = jnp.zeros((CH, B), f32)
    put_source(0, None, None)
    green_from(0, lambda stage: None)

    def forward_step(i, carry):
        kind = bk_ref[i - 1]
        v = jnp.where(kind == 0, couplings[0], jnp.where(kind == 1, couplings[1], couplings[2]))
        put(vv, (slice(None),), v)
        put(vt, (slice(None),), v.T)
        p = dot3(get(gs, both), get(vv))
        for r, a, b in chunks():
            put3(pr, (i - 1,), r, 2 * B, p[a], p[b], False)
        lesser_left()
        part = lambda j: dot3(get(vt), get(pr, i - 1, pl.ds((0, 2, 1, 3)[j] * B, B)))
        m = part(0), part(1)
        for r, a, _ in chunks():
            mf[0, pl.ds(r, CH)] = -onsite[i, pl.ds(r, CH)] - m[0][a]
            mf[1, pl.ds(r, CH)] = -m[1][a]
        lesser_of(i - 1)

        def between(stage):
            if stage == 0:
                q = dot3(get(ws, both), get(vv))
                for r, a, b in chunks():
                    put3(pr, (i - 1,), B + r, 2 * B, q[a], q[b], True)
            else:
                put_source(i, part(2), part(3))

        green_from(i, between)
        return carry

    for copy in copies[3:]:
        copy.wait()
    lax.fori_loop(1, layers + 1, forward_step, 0)
    pl.semaphore_wait(barrier, len(peers))
    lesser_left()
    lesser_of(layers)
    hf[...] = jnp.zeros_like(hf)

    def report(i, m, r, x):
        if i == layers:
            return
        x = weight * x
        for half in range(0, CH, 16):
            e = (r + half) // 16
            blocks[i, m, e // 4, e // 2 % 2, e % 2] = x[half : half + 16]

    def finish(i, last):
        h_re, h_im = hf[0].T, hf[1].T
        for r, a, _ in chunks():
            w_re = wf[i, pl.ds(r, CH)] + (hf[0, pl.ds(r, CH)] + h_re[a])
            w_im = wf[i, pl.ds(B + r, CH)] + (hf[1, pl.ds(r, CH)] - h_im[a])
            report(i, 0, r, w_re)
            report(i, 1, r, w_im)
            if not last:
                put3(ws, (), r, B, w_re, w_im, False)

    def backward(i, inner):
        from_left = lambda n: get(pr, i, pl.ds(2 * n * B, B))
        from_right = lambda n: get(pr, i, pl.ds((2 * n + 1) * B, B))
        if inner:
            q = product(from_left, thirds(gs))
        z = product(from_right, thirds(gs), True)
        finish(i + 1, False)
        if i < layers - 1:
            core_start(i + 1)
        pw = product(from_left, thirds(ws))
        if inner:
            for r, a, _ in chunks():
                put3(al, (), r, B, *q(a), False)
            grown = product(thirds(al), from_left, False, True)
        for r, a, _ in chunks():
            (p_re, p_im), (z_re, z_im) = pw(a), z(a)
            report(i, 2, r, p_re + z_re)
            report(i, 3, r, p_im + z_im)
            put3(ml, (), r, B, 0.5 * p_re + z_re, 0.5 * p_im + z_im, True)
        if inner:
            for r, a, _ in chunks():
                n_re, n_im = grown(a)
                put3(gs, (), r, B, gf[i, pl.ds(r, CH)] + n_re, gf[i, pl.ds(B + r, CH)] + n_im, False)
        h = product(thirds(ml), from_left, True, True)
        for r, a, _ in chunks():
            hf[0, pl.ds(r, CH)], hf[1, pl.ds(r, CH)] = h(a)
        if i == 0:
            plane_turn(3)
        if i < layers - 1:
            core_finish(i + 1)
            plane_start(i + 1)

    backward(3, True)
    for i in (2, 1, 0):
        backward(i, i > 0)
    finish(0, True)
    core_start(0)
    plane_turn(2)
    core_finish(0)
    plane_start(0)
    plane_finish(3)
    line_start(3)
    plane_turn(1)
    plane_finish(2)
    line_start(2)
    plane_turn(0)
    plane_finish(1)
    line_start(1)
    for i in (3, 2, 1):
        line_finish(i)
    plane_finish(0)
    line_start(0)
    line_finish(0)
    owner_exchange()
    for i in range(layers):
        wait(from_core.at[i], core_sems.at[0, i])
        for way in range(2):
            wait(from_first.at[i, way], first_sems.at[0, way, i])
            wait(from_second.at[i, way], second_sems.at[0, way, i])
        wait(from_line.at[i], line_sems.at[0, i])
    wait(many, owner_sems.at[0])


def scratch(layers):
    pair = lambda *s: [pltpu.VMEM(s, bf16), pltpu.VMEM(s, bf16)]
    full = lambda *s: pltpu.VMEM(s, f32)
    three = pair(3 * B, B)
    return (
        three + three + pair(layers, 6 * B, B) + three + three + three + three + three
        + pair(B, B) + pair(B, B)
        + [full(layers + 1, 2 * B, B)] * 2 + [full(2, B, B)] * 2
        + [
            full(layers, 4, 4, 2, 2, 16, B),
            full(layers, 4, 4, 2, 16, B),
            full(layers, 4, 4, 2, 16, B),
            full(layers, 2, 3, 4, 16, B),
            full(layers, 2, 4, 16, B),
            full(layers, 2, 3, 16, B),
            full(layers, 2, 4, 8, 128),
            full(layers, 7, 8, 128),
            full(layers, 8, 128),
            full(15, 8, 128),
            pltpu.SemaphoreType.DMA((2, layers)),
            pltpu.SemaphoreType.DMA((2, 2, layers)),
            pltpu.SemaphoreType.DMA((2, 2, layers)),
            pltpu.SemaphoreType.DMA((2, layers)),
            pltpu.SemaphoreType.DMA((3,)),
        ]
    )


def per_device(
    energies, momenta, energy_level, momentum_level, energy_table, momentum_table,
    onsite, broad, kdiag, fermi, couplings, bond_kind,
):
    layers = onsite.shape[0] - 1
    args = (
        energies, momenta, energy_level, momentum_level, energy_table, momentum_table,
        fermi, bond_kind, broad, kdiag, couplings, onsite,
    )
    held = [pltpu.VMEM(x.shape, x.dtype) for x in args[8:]]
    owned = pl.pallas_call(
        sweeps,
        out_shape=jax.ShapeDtypeStruct((4, 2, 8, B), f32),
        in_specs=[pl.BlockSpec(memory_space=pltpu.SMEM)] * 8 + [pl.BlockSpec(memory_space=pl.ANY)] * 4,
        out_specs=pl.BlockSpec(memory_space=pl.ANY),
        scratch_shapes=held + [pltpu.SemaphoreType.DMA((5,))] + scratch(layers),
        compiler_params=pltpu.CompilerParams(
            vmem_limit_bytes=62 << 20, collective_id=0, has_side_effects=True
        ),
        name="sweeps",
    )(*args).reshape(4, 16, B)
    return owned[None, :2], owned[None, 2:]


def solution(mesh):
    rep = P()
    both = P(("energy", "layer"))
    return jax.shard_map(
        per_device,
        mesh=mesh,
        in_specs=(both, P("kpt"), both, P("kpt"), rep, rep, rep, rep, rep, rep, rep, rep),
        out_specs=(P("layer", None, "energy", None), P("layer", None, "energy", None)),
        check_vma=False,
    )
```

```python
import jax
import jax.numpy as jnp
from jax import lax
from jax.experimental import pallas as pl
from jax.experimental.pallas import tpu as pltpu
from jax.sharding import PartitionSpec as P

bf16 = jnp.bfloat16
f32 = jnp.float32
B = 256
CH = 32


def dot(a, b, tb=False):
    return lax.dot_general(
        a, b, (((1,), (1 if tb else 0,)), ((), ())), preferred_element_type=f32
    )


def split(x):
    high = x.astype(bf16)
    return high, (x - high.astype(f32)).astype(bf16)


def dot3(left, right, tb=False):
    return (
        dot(left[0], right[0], tb) + dot(left[0], right[1], tb) + dot(left[1], right[0], tb)
    )


def get(pair, *at):
    return pair[0][at], pair[1][at]


def put(pair, at, x):
    pair[0][at], pair[1][at] = split(x)


def put3(pair, lead, at, stride, re, im, conj):
    for n, x in enumerate((re, im, re - im if conj else re + im)):
        put(pair, lead + (pl.ds(at + n * stride, CH),), x)


def product(left, right, conj=False, tb=False):
    t1, t2, t3 = (dot3(left(n), right(n), tb) for n in range(3))

    def rows(a):
        if conj:
            return t1[a] + t2[a], (t1[a] - t2[a]) - t3[a]
        return t1[a] - t2[a], t3[a] - (t1[a] + t2[a])

    return rows


def thirds(pair, *lead):
    return lambda n: get(pair, *lead, pl.ds(n * B, B))


def chunks():
    for r in range(0, B, CH):
        yield r, slice(r, r + CH), slice(B + r, B + r + CH)


def sweeps(
    *refs,
):
    scalars, inputs, result = refs[:8], refs[8:12], refs[12]
    held, in_sems, rest = refs[13:17], refs[17], refs[18:]
    broad, kdiag, couplings, onsite = zip(inputs, held)
    first, rest_of = pl.ds(0, 1), pl.ds(1, onsite[0].shape[0] - 1)
    pairs = [broad, kdiag, [x.at[first] for x in onsite], couplings, [x.at[rest_of] for x in onsite]]
    copies = [pltpu.make_async_copy(a, b, in_sems.at[n]) for n, (a, b) in enumerate(pairs)]
    for copy in copies:
        copy.start()
    sweep_body(copies, result, *scalars, *held, *rest)


def sweep_body(
    copies, result, e_ref, k_ref, el_ref, ml_ref, et_ref, mt_ref, fermi_ref, bk_ref,
    broad, kdiag, couplings, onsite,
    gs_h, gs_l, ws_h, ws_l, pr_h, pr_l, al_h, al_l, ul_h, ul_l, ss_h, ss_l,
    tl_h, tl_l, ml_h, ml_l, v_h, v_l, vt_h, vt_l, gf, wf, mf, hf,
    blocks, from_core, rows_x, tiles_y, from_x, from_y, second, from_second, to_line, from_line, to_owner, many,
    core_sems, first_sems, second_sems, line_sems, owner_sems,
):
    layers = onsite.shape[0] - 1
    gs, ws, pr, al, ul, ss, tl, ml, vv, vt = (
        (gs_h, gs_l), (ws_h, ws_l), (pr_h, pr_l), (al_h, al_l), (ul_h, ul_l),
        (ss_h, ss_l), (tl_h, tl_l), (ml_h, ml_l), (v_h, v_l), (vt_h, vt_l),
    )
    energy = e_ref[0]
    moment = k_ref[0]
    weight = et_ref[el_ref[0]] * mt_ref[ml_ref[0]] * (1.0 / 256)
    me_e, me_k, me_l = lax.axis_index("energy"), lax.axis_index("kpt"), lax.axis_index("layer")
    me_x, me_z, me_c = lax.div(me_e, 4), lax.rem(lax.div(me_e, 2), 2), lax.rem(me_e, 2)

    def device(x, z, c, k, y):
        return ((x * 2 + z) * 2 + c, k, y)

    def core_peer():
        return device(me_x, me_z, 1 - me_c, me_k, me_l)

    def after(at, step):
        return lax.rem(at + step, 4)

    def x_device(step):
        return device(after(me_x, step), me_z, me_c, me_k, me_l)

    def y_device(step):
        return device(me_x, me_z, me_c, me_k, after(me_l, step))

    def line_peer(step):
        return lax.rem(me_z + step // 4, 2), lax.rem(me_k + step % 4, 4)

    def owner_peer(step):
        return lax.rem(me_k + step // 4, 4), lax.rem(me_l + step % 4, 4)

    def line_device(step):
        z, k = line_peer(step)
        return device(me_x, z, me_c, k, me_l)

    def owner_device(step):
        k, y = owner_peer(step)
        return device(me_x, me_z, me_c, k, y)

    barrier = pltpu.get_barrier_semaphore()
    peers = [core_peer()] + [x_device(s) for s in range(1, 4)]
    peers += [line_device(s) for s in range(1, 8)] + [owner_device(s) for s in range(1, 16)]
    for peer in peers:
        pl.semaphore_signal(barrier, inc=1, device_id=peer, device_id_type=pl.DeviceIdType.MESH)

    def send(src, dst, sems, peer):
        pltpu.make_async_remote_copy(
            src_ref=src, dst_ref=dst, send_sem=sems[0], recv_sem=sems[1],
            device_id=peer, device_id_type=pl.DeviceIdType.MESH,
        ).start()

    def wait(like, sem):
        pltpu.make_async_copy(like, like, sem).wait()

    def core_start(i):
        send(blocks.at[i, :, :, :, 1 - me_c], from_core.at[i],
             (core_sems.at[0, i], core_sems.at[1, i]), core_peer())

    def core_finish(i):
        wait(from_core.at[i], core_sems.at[1, i])
        for m in range(4):
            for x in range(4):
                rows_x[i, m, x] = blocks[i, m, x, 0, me_c] + from_core[i, m, x, 0]
                other = blocks[i, m, x, 1, me_c] + from_core[i, m, x, 1]
                for k in range(4):
                    row, col = 8 * (k // 2), 128 * (k % 2)
                    tiles_y[i, m, x, k] = other[row : row + 8, col : col + 128]

    def plane_start(i):
        for step in range(1, 4):
            send(rows_x.at[i, :, after(me_x, step)], from_x.at[i, step - 1],
                 (first_sems.at[0, 0, i], first_sems.at[1, 0, i]), x_device(step))
            send(tiles_y.at[i, :, :, after(me_l, step)], from_y.at[i, step - 1],
                 (first_sems.at[0, 1, i], first_sems.at[1, 1, i]), y_device(step))

    def plane_gather(i):
        wait(from_x.at[i], first_sems.at[1, 0, i])
        for m in range(4):
            total = rows_x[i, m, me_x] + from_x[i, 0, m] + (from_x[i, 1, m] + from_x[i, 2, m])
            for k in range(4):
                row, col = 8 * (k // 2), 128 * (k % 2)
                second[i, 0, m, k] = total[row : row + 8, col : col + 128]
        wait(from_y.at[i], first_sems.at[1, 1, i])
        for m in range(4):
            second[i, 1, m] = tiles_y[i, m, :, me_l] + from_y[i, 0, m] + (
                from_y[i, 1, m] + from_y[i, 2, m]
            )

    def plane_turn(lo, n):
        some = pl.ds(lo, n)
        for step in range(1, 4):
            send(second.at[some, 0, :, after(me_l, step)], from_second.at[some, 0, step - 1],
                 (second_sems.at[0, 0, lo], second_sems.at[1, 0, lo]), y_device(step))
            send(second.at[some, 1, :, after(me_x, step)], from_second.at[some, 1, step - 1],
                 (second_sems.at[0, 1, lo], second_sems.at[1, 1, lo]), x_device(step))

    def line_start(lo, n):
        some = pl.ds(lo, n)
        for z in range(2):
            wait(from_second.at[some, z], second_sems.at[1, z, lo])
            for i in range(lo, lo + n):
                for m in range(4):
                    own = second[i, z, m, me_l if z == 0 else me_x]
                    to_line[i, z, m] = own + from_second[i, z, 0, m] + (
                        from_second[i, z, 1, m] + from_second[i, z, 2, m]
                    )
        for step in range(1, 8):
            z, k = line_peer(step)
            send(to_line.at[some, z, k], from_line.at[some, step - 1],
                 (line_sems.at[0, lo], line_sems.at[1, lo]), line_device(step))

    def line_finish(lo, n):
        wait(from_line.at[pl.ds(lo, n)], line_sems.at[1, lo])
        for i in range(lo, lo + n):
            total = to_line[i, me_z, me_k]
            for step in range(1, 8):
                total = total + from_line[i, step - 1]
            to_owner[i] = total

    def owner_exchange():
        mine = result.at[me_k, lax.div(me_l, 2), :, pl.ds(pl.multiple_of(128 * lax.rem(me_l, 2), 128), 128)]
        for step in range(1, 16):
            k, y = owner_peer(step)
            send(to_owner.at[y], mine, (owner_sems.at[0], owner_sems.at[1]), owner_device(step))
        own = pltpu.make_async_copy(to_owner.at[me_l], mine, owner_sems.at[2])
        own.start()
        own.wait()
        wait(many, owner_sems.at[1])

    for copy in copies[:3]:
        copy.wait()
    both = pl.ds(0, 2 * B)

    def diagonal_of(r, lanes):
        at = r % 128 if lanes == 128 else r
        return (
            lax.broadcasted_iota(jnp.int32, (CH, lanes), 0) + at
            == lax.broadcasted_iota(jnp.int32, (CH, lanes), 1)
        )

    def source(i):
        br = broad[pl.ds(i, 1), :]
        return br * jax.nn.sigmoid(jnp.full((1, B), (fermi_ref[i] - energy) / 0.25, f32))

    def inverse_ends(i):
        shift = energy - moment * kdiag[pl.ds(i, 1), :]
        half = 0.5 * broad[pl.ds(i, 1), :]
        rows = []
        cols = {}
        for t in range(2):
            lane = slice(128 * t, 128 * t + 128)
            dr_row = di_row = 0.0
            for r in range(128 * t, 128 * t + 128, CH):
                on = diagonal_of(r, 128)
                dr = jnp.where(on, mf[0, pl.ds(r, CH), lane] + shift[:, lane], 0.0)
                di = jnp.where(on, mf[1, pl.ds(r, CH), lane] + half[:, lane], 0.0)
                dr_row = dr_row + jnp.sum(dr, 0, keepdims=True)
                di_row = di_row + jnp.sum(di, 0, keepdims=True)
                a, b = jnp.sum(dr, 1, keepdims=True), jnp.sum(di, 1, keepdims=True)
                n = 1.0 / (a * a + b * b)
                cols[r] = (a * n, -b * n)
            n = 1.0 / (dr_row * dr_row + di_row * di_row)
            rows.append((dr_row * n, -di_row * n))
        return tuple(jnp.concatenate([rows[0][c], rows[1][c]], 1) for c in range(2)), cols

    def green_from(i, between):
        (rr, ri), cols = inverse_ends(i)
        for r, _, _ in chunks():
            on = diagonal_of(r, B)
            m_re = jnp.where(on, 0.0, mf[0, pl.ds(r, CH)])
            m_im = jnp.where(on, 0.0, mf[1, pl.ds(r, CH)])
            cr, ci = cols[r]
            a_re = cr * m_re - ci * m_im
            a_im = cr * m_im + ci * m_re
            put3(al, (), r, B, a_re, a_im, False)
            mf[0, pl.ds(r, CH)] = jnp.where(on, 1.0, 0.0) - a_re
            mf[1, pl.ds(r, CH)] = -a_im
        sq = product(thirds(al), thirds(al))
        between(0)
        for r, a, _ in chunks():
            u_re, u_im = sq(a)
            put3(ul, (), r, B, u_re, u_im, False)
            mf[0, pl.ds(r, CH)] += u_re
            mf[1, pl.ds(r, CH)] += u_im
        cube = product(thirds(ul), thirds(al))
        between(1)
        for r, a, _ in chunks():
            c_re, c_im = cube(a)
            t_re = mf[0, pl.ds(r, CH)] - c_re
            t_im = mf[1, pl.ds(r, CH)] - c_im
            g_re = t_re * rr - t_im * ri
            g_im = t_re * ri + t_im * rr
            gf[i, pl.ds(r, CH)] = g_re
            gf[i, pl.ds(B + r, CH)] = g_im
            put3(gs, (), r, B, g_re, g_im, False)

    def put_source(i, s_re, s_im):
        gamma = source(i)
        for r, a, _ in chunks():
            x = jnp.where(diagonal_of(r, B), gamma, 0.0)
            if s_re is not None:
                x = x + s_re[a]
            put3(ss, (), r, B, x, jnp.zeros((CH, B), f32) if s_im is None else s_im[a], False)

    def lesser_left():
        t = product(thirds(gs), thirds(ss))
        for r, a, _ in chunks():
            put3(tl, (), r, B, *t(a), True)

    def lesser_of(i):
        w = product(thirds(tl), thirds(gs), True)
        for r, a, _ in chunks():
            w_re, w_im = w(a)
            wf[i, pl.ds(r, CH)] = w_re
            wf[i, pl.ds(B + r, CH)] = w_im
            put(ws, (pl.ds(r, CH),), w_re)
            put(ws, (pl.ds(B + r, CH),), w_im)

    for r, _, _ in chunks():
        mf[0, pl.ds(r, CH)] = -onsite[0, pl.ds(r, CH)]
        mf[1, pl.ds(r, CH)] = jnp.zeros((CH, B), f32)
    put_source(0, None, None)
    green_from(0, lambda stage: None)

    def forward_step(i, carry):
        kind = bk_ref[i - 1]
        v = jnp.where(kind == 0, couplings[0], jnp.where(kind == 1, couplings[1], couplings[2]))
        put(vv, (slice(None),), v)
        put(vt, (slice(None),), v.T)
        p = dot3(get(gs, both), get(vv))
        for r, a, b in chunks():
            put3(pr, (i - 1,), r, 2 * B, p[a], p[b], False)
        lesser_left()
        part = lambda j: dot3(get(vt), get(pr, i - 1, pl.ds((0, 2, 1, 3)[j] * B, B)))
        m = part(0), part(1)
        for r, a, _ in chunks():
            mf[0, pl.ds(r, CH)] = -onsite[i, pl.ds(r, CH)] - m[0][a]
            mf[1, pl.ds(r, CH)] = -m[1][a]
        lesser_of(i - 1)

        def between(stage):
            if stage == 0:
                q = dot3(get(ws, both), get(vv))
                for r, a, b in chunks():
                    put3(pr, (i - 1,), B + r, 2 * B, q[a], q[b], True)
            else:
                put_source(i, part(2), part(3))

        green_from(i, between)
        return carry

    for copy in copies[3:]:
        copy.wait()
    lax.fori_loop(1, layers + 1, forward_step, 0)
    pl.semaphore_wait(barrier, len(peers))
    lesser_left()
    lesser_of(layers)
    hf[...] = jnp.zeros_like(hf)

    def report(i, m, r, x):
        if i == layers:
            return
        x = weight * x
        for half in range(0, CH, 16):
            e = (r + half) // 16
            blocks[i, m, e // 4, e // 2 % 2, e % 2] = x[half : half + 16]

    def finish(i, last):
        h_re, h_im = hf[0].T, hf[1].T
        for r, a, _ in chunks():
            w_re = wf[i, pl.ds(r, CH)] + (hf[0, pl.ds(r, CH)] + h_re[a])
            w_im = wf[i, pl.ds(B + r, CH)] + (hf[1, pl.ds(r, CH)] - h_im[a])
            report(i, 0, r, w_re)
            report(i, 1, r, w_im)
            if not last:
                put3(ws, (), r, B, w_re, w_im, False)

    def backward(i, inner):
        from_left = lambda n: get(pr, i, pl.ds(2 * n * B, B))
        from_right = lambda n: get(pr, i, pl.ds((2 * n + 1) * B, B))
        if inner:
            q = product(from_left, thirds(gs))
        z = product(from_right, thirds(gs), True)
        finish(i + 1, False)
        if i < layers - 1:
            core_start(i + 1)
        pw = product(from_left, thirds(ws))
        if inner:
            for r, a, _ in chunks():
                put3(al, (), r, B, *q(a), False)
            grown = product(thirds(al), from_left, False, True)
        for r, a, _ in chunks():
            (p_re, p_im), (z_re, z_im) = pw(a), z(a)
            report(i, 2, r, p_re + z_re)
            report(i, 3, r, p_im + z_im)
            put3(ml, (), r, B, 0.5 * p_re + z_re, 0.5 * p_im + z_im, True)
        if inner:
            for r, a, _ in chunks():
                n_re, n_im = grown(a)
                put3(gs, (), r, B, gf[i, pl.ds(r, CH)] + n_re, gf[i, pl.ds(B + r, CH)] + n_im, False)
        h = product(thirds(ml), from_left, True, True)
        for r, a, _ in chunks():
            hf[0, pl.ds(r, CH)], hf[1, pl.ds(r, CH)] = h(a)
        if i < layers - 1:
            core_finish(i + 1)
            plane_start(i + 1)

    backward(3, True)
    for i in (2, 1, 0):
        backward(i, i > 0)
    finish(0, True)
    core_start(0)
    plane_gather(3)
    plane_gather(2)
    core_finish(0)
    plane_start(0)
    plane_gather(1)
    plane_turn(1, 3)
    plane_gather(0)
    plane_turn(0, 1)
    line_start(1, 3)
    line_start(0, 1)
    line_finish(1, 3)
    line_finish(0, 1)
    owner_exchange()
    for i in range(layers):
        wait(from_core.at[i], core_sems.at[0, i])
        wait(from_x.at[i], first_sems.at[0, 0, i])
        wait(from_y.at[i], first_sems.at[0, 1, i])
    for lo, n in ((0, 1), (1, 3)):
        some = pl.ds(lo, n)
        for way in range(2):
            wait(from_second.at[some, way], second_sems.at[0, way, lo])
        wait(from_line.at[some], line_sems.at[0, lo])
    wait(many, owner_sems.at[0])


def scratch(layers):
    pair = lambda *s: [pltpu.VMEM(s, bf16), pltpu.VMEM(s, bf16)]
    full = lambda *s: pltpu.VMEM(s, f32)
    three = pair(3 * B, B)
    return (
        three + three + pair(layers, 6 * B, B) + three + three + three + three + three
        + pair(B, B) + pair(B, B)
        + [full(layers + 1, 2 * B, B)] * 2 + [full(2, B, B)] * 2
        + [
            full(layers, 4, 4, 2, 2, 16, B),
            full(layers, 4, 4, 2, 16, B),
            full(layers, 4, 4, 16, B),
            full(layers, 4, 4, 4, 8, 128),
            full(layers, 3, 4, 16, B),
            full(layers, 3, 4, 4, 8, 128),
            full(layers, 2, 4, 4, 8, 128),
            full(layers, 2, 3, 4, 8, 128),
            full(layers, 2, 4, 8, 128),
            full(layers, 7, 8, 128),
            full(layers, 8, 128),
            full(15, 8, 128),
            pltpu.SemaphoreType.DMA((2, layers)),
            pltpu.SemaphoreType.DMA((2, 2, layers)),
            pltpu.SemaphoreType.DMA((2, 2, 2)),
            pltpu.SemaphoreType.DMA((2, 2)),
            pltpu.SemaphoreType.DMA((3,)),
        ]
    )


def per_device(
    energies, momenta, energy_level, momentum_level, energy_table, momentum_table,
    onsite, broad, kdiag, fermi, couplings, bond_kind,
):
    layers = onsite.shape[0] - 1
    args = (
        energies, momenta, energy_level, momentum_level, energy_table, momentum_table,
        fermi, bond_kind, broad, kdiag, couplings, onsite,
    )
    held = [pltpu.VMEM(x.shape, x.dtype) for x in args[8:]]
    owned = pl.pallas_call(
        sweeps,
        out_shape=jax.ShapeDtypeStruct((4, 2, 8, B), f32),
        in_specs=[pl.BlockSpec(memory_space=pltpu.SMEM)] * 8 + [pl.BlockSpec(memory_space=pl.ANY)] * 4,
        out_specs=pl.BlockSpec(memory_space=pl.ANY),
        scratch_shapes=held + [pltpu.SemaphoreType.DMA((5,))] + scratch(layers),
        compiler_params=pltpu.CompilerParams(
            vmem_limit_bytes=62 << 20, collective_id=0, has_side_effects=True
        ),
        name="sweeps",
    )(*args).reshape(4, 16, B)
    return owned[None, :2], owned[None, 2:]


def solution(mesh):
    rep = P()
    both = P(("energy", "layer"))
    return jax.shard_map(
        per_device,
        mesh=mesh,
        in_specs=(both, P("kpt"), both, P("kpt"), rep, rep, rep, rep, rep, rep, rep, rep),
        out_specs=(P("layer", None, "energy", None), P("layer", None, "energy", None)),
        check_vma=False,
    )
```

```python
import jax
import jax.numpy as jnp
from jax import lax
from jax.experimental import pallas as pl
from jax.experimental.pallas import tpu as pltpu
from jax.sharding import PartitionSpec as P

bf16 = jnp.bfloat16
f32 = jnp.float32
B = 256
CH = 32


def dot(a, b, tb=False):
    return lax.dot_general(
        a, b, (((1,), (1 if tb else 0,)), ((), ())), preferred_element_type=f32
    )


def split(x):
    high = x.astype(bf16)
    return high, (x - high.astype(f32)).astype(bf16)


def dot3(left, right, tb=False):
    return (
        dot(left[0], right[0], tb) + dot(left[0], right[1], tb) + dot(left[1], right[0], tb)
    )


def get(pair, *at):
    return pair[0][at], pair[1][at]


def put(pair, at, x):
    pair[0][at], pair[1][at] = split(x)


def put3(pair, lead, at, stride, re, im, conj):
    for n, x in enumerate((re, im, re - im if conj else re + im)):
        put(pair, lead + (pl.ds(at + n * stride, CH),), x)


def product(left, right, conj=False, tb=False):
    t1, t2, t3 = (dot3(left(n), right(n), tb) for n in range(3))

    def rows(a):
        if conj:
            return t1[a] + t2[a], (t1[a] - t2[a]) - t3[a]
        return t1[a] - t2[a], t3[a] - (t1[a] + t2[a])

    return rows


def thirds(pair, *lead):
    return lambda n: get(pair, *lead, pl.ds(n * B, B))


def chunks():
    for r in range(0, B, CH):
        yield r, slice(r, r + CH), slice(B + r, B + r + CH)


def sweeps(
    *refs,
):
    scalars, inputs, result = refs[:8], refs[8:12], refs[12]
    held, in_sems, rest = refs[13:17], refs[17], refs[18:]
    broad, kdiag, couplings, onsite = zip(inputs, held)
    first, rest_of = pl.ds(0, 1), pl.ds(1, onsite[0].shape[0] - 1)
    pairs = [broad, kdiag, [x.at[first] for x in onsite], couplings, [x.at[rest_of] for x in onsite]]
    copies = [pltpu.make_async_copy(a, b, in_sems.at[n]) for n, (a, b) in enumerate(pairs)]
    for copy in copies:
        copy.start()
    sweep_body(copies, result, *scalars, *held, *rest)


def sweep_body(
    copies, result, e_ref, k_ref, el_ref, ml_ref, et_ref, mt_ref, fermi_ref, bk_ref,
    broad, kdiag, couplings, onsite,
    gs_h, gs_l, ws_h, ws_l, pr_h, pr_l, al_h, al_l, ul_h, ul_l, ss_h, ss_l,
    tl_h, tl_l, ml_h, ml_l, v_h, v_l, vt_h, vt_l, gf, wf, mf, hf,
    blocks, from_core, rows_x, tiles_y, from_x, from_y, second, from_second, to_line, from_line, to_owner, many,
    core_sems, first_sems, second_sems, line_sems, owner_sems,
):
    layers = onsite.shape[0] - 1
    gs, ws, pr, al, ul, ss, tl, ml, vv, vt = (
        (gs_h, gs_l), (ws_h, ws_l), (pr_h, pr_l), (al_h, al_l), (ul_h, ul_l),
        (ss_h, ss_l), (tl_h, tl_l), (ml_h, ml_l), (v_h, v_l), (vt_h, vt_l),
    )
    energy = e_ref[0]
    moment = k_ref[0]
    weight = et_ref[el_ref[0]] * mt_ref[ml_ref[0]] * (1.0 / 256)
    me_e, me_k, me_l = lax.axis_index("energy"), lax.axis_index("kpt"), lax.axis_index("layer")
    me_x, me_z, me_c = lax.div(me_e, 4), lax.rem(lax.div(me_e, 2), 2), lax.rem(me_e, 2)

    def device(x, z, c, k, y):
        return ((x * 2 + z) * 2 + c, k, y)

    def core_peer():
        return device(me_x, me_z, 1 - me_c, me_k, me_l)

    def after(at, step):
        return lax.rem(at + step, 4)

    def x_device(step):
        return device(after(me_x, step), me_z, me_c, me_k, me_l)

    def y_device(step):
        return device(me_x, me_z, me_c, me_k, after(me_l, step))

    def line_peer(step):
        return lax.rem(me_z + step // 4, 2), lax.rem(me_k + step % 4, 4)

    def owner_peer(step):
        return lax.rem(me_k + step // 4, 4), lax.rem(me_l + step % 4, 4)

    def line_device(step):
        z, k = line_peer(step)
        return device(me_x, z, me_c, k, me_l)

    def owner_device(step):
        k, y = owner_peer(step)
        return device(me_x, me_z, me_c, k, y)

    barrier = pltpu.get_barrier_semaphore()
    peers = [core_peer()] + [x_device(s) for s in range(1, 4)]
    peers += [line_device(s) for s in range(1, 8)] + [owner_device(s) for s in range(1, 16)]
    for peer in peers:
        pl.semaphore_signal(barrier, inc=1, device_id=peer, device_id_type=pl.DeviceIdType.MESH)

    def send(src, dst, sems, peer):
        pltpu.make_async_remote_copy(
            src_ref=src, dst_ref=dst, send_sem=sems[0], recv_sem=sems[1],
            device_id=peer, device_id_type=pl.DeviceIdType.MESH,
        ).start()

    def wait(like, sem):
        pltpu.make_async_copy(like, like, sem).wait()

    def core_start(i):
        send(blocks.at[i, :, :, :, 1 - me_c], from_core.at[i],
             (core_sems.at[0, i], core_sems.at[1, i]), core_peer())

    def core_finish(i):
        wait(from_core.at[i], core_sems.at[1, i])
        for m in range(4):
            for x in range(4):
                rows_x[i, m, x] = blocks[i, m, x, 0, me_c] + from_core[i, m, x, 0]
                other = blocks[i, m, x, 1, me_c] + from_core[i, m, x, 1]
                for k in range(4):
                    row, col = 8 * (k // 2), 128 * (k % 2)
                    tiles_y[i, m, x, k] = other[row : row + 8, col : col + 128]

    def plane_start(i):
        for step in range(1, 4):
            send(rows_x.at[i, :, after(me_x, step)], from_x.at[i, step - 1],
                 (first_sems.at[0, 0, i], first_sems.at[1, 0, i]), x_device(step))
            send(tiles_y.at[i, :, :, after(me_l, step)], from_y.at[i, step - 1],
                 (first_sems.at[0, 1, i], first_sems.at[1, 1, i]), y_device(step))

    def plane_gather(i):
        wait(from_x.at[i], first_sems.at[1, 0, i])
        for m in range(4):
            total = rows_x[i, m, me_x] + from_x[i, 0, m] + (from_x[i, 1, m] + from_x[i, 2, m])
            for k in range(4):
                row, col = 8 * (k // 2), 128 * (k % 2)
                second[i, 0, m, k] = total[row : row + 8, col : col + 128]
        wait(from_y.at[i], first_sems.at[1, 1, i])
        for m in range(4):
            second[i, 1, m] = tiles_y[i, m, :, me_l] + from_y[i, 0, m] + (
                from_y[i, 1, m] + from_y[i, 2, m]
            )

    def plane_turn(lo, n):
        some = pl.ds(lo, n)
        for step in range(1, 4):
            send(second.at[some, 0, :, after(me_l, step)], from_second.at[some, 0, step - 1],
                 (second_sems.at[0, 0, lo], second_sems.at[1, 0, lo]), y_device(step))
            send(second.at[some, 1, :, after(me_x, step)], from_second.at[some, 1, step - 1],
                 (second_sems.at[0, 1, lo], second_sems.at[1, 1, lo]), x_device(step))

    def line_start(lo, n):
        some = pl.ds(lo, n)
        for z in range(2):
            wait(from_second.at[some, z], second_sems.at[1, z, lo])
            for i in range(lo, lo + n):
                for m in range(4):
                    own = second[i, z, m, me_l if z == 0 else me_x]
                    to_line[i, z, m] = own + from_second[i, z, 0, m] + (
                        from_second[i, z, 1, m] + from_second[i, z, 2, m]
                    )
        for step in range(1, 8):
            z, k = line_peer(step)
            send(to_line.at[some, z, k], from_line.at[some, step - 1],
                 (line_sems.at[0, lo], line_sems.at[1, lo]), line_device(step))

    def line_finish(lo, n):
        wait(from_line.at[pl.ds(lo, n)], line_sems.at[1, lo])
        for i in range(lo, lo + n):
            total = to_line[i, me_z, me_k]
            for step in range(1, 8):
                total = total + from_line[i, step - 1]
            to_owner[i] = total

    mine = result.at[
        me_k, lax.div(me_l, 2), :, pl.ds(pl.multiple_of(128 * lax.rem(me_l, 2), 128), 128)
    ]

    def owner_send(k, y):
        send(to_owner.at[y], mine, (owner_sems.at[0], owner_sems.at[1]),
             device(me_x, me_z, me_c, k, y))

    def owners_above():
        for step in range(1, 16):
            k, y = owner_peer(step)

            @pl.when(y != 0)
            def _():
                owner_send(k, y)

    def owner_exchange():
        for step in range(1, 4):
            owner_send(after(me_k, step), 0)

        @pl.when(me_l != 0)
        def _():
            owner_send(me_k, 0)

        own = pltpu.make_async_copy(to_owner.at[me_l], mine, owner_sems.at[2])
        own.start()
        own.wait()
        wait(many, owner_sems.at[1])

    for copy in copies[:3]:
        copy.wait()
    both = pl.ds(0, 2 * B)

    def diagonal_of(r, lanes):
        at = r % 128 if lanes == 128 else r
        return (
            lax.broadcasted_iota(jnp.int32, (CH, lanes), 0) + at
            == lax.broadcasted_iota(jnp.int32, (CH, lanes), 1)
        )

    def source(i):
        br = broad[pl.ds(i, 1), :]
        return br * jax.nn.sigmoid(jnp.full((1, B), (fermi_ref[i] - energy) / 0.25, f32))

    def inverse_ends(i):
        shift = energy - moment * kdiag[pl.ds(i, 1), :]
        half = 0.5 * broad[pl.ds(i, 1), :]
        rows = []
        cols = {}
        for t in range(2):
            lane = slice(128 * t, 128 * t + 128)
            dr_row = di_row = 0.0
            for r in range(128 * t, 128 * t + 128, CH):
                on = diagonal_of(r, 128)
                dr = jnp.where(on, mf[0, pl.ds(r, CH), lane] + shift[:, lane], 0.0)
                di = jnp.where(on, mf[1, pl.ds(r, CH), lane] + half[:, lane], 0.0)
                dr_row = dr_row + jnp.sum(dr, 0, keepdims=True)
                di_row = di_row + jnp.sum(di, 0, keepdims=True)
                a, b = jnp.sum(dr, 1, keepdims=True), jnp.sum(di, 1, keepdims=True)
                n = 1.0 / (a * a + b * b)
                cols[r] = (a * n, -b * n)
            n = 1.0 / (dr_row * dr_row + di_row * di_row)
            rows.append((dr_row * n, -di_row * n))
        return tuple(jnp.concatenate([rows[0][c], rows[1][c]], 1) for c in range(2)), cols

    def green_from(i, between):
        (rr, ri), cols = inverse_ends(i)
        for r, _, _ in chunks():
            on = diagonal_of(r, B)
            m_re = jnp.where(on, 0.0, mf[0, pl.ds(r, CH)])
            m_im = jnp.where(on, 0.0, mf[1, pl.ds(r, CH)])
            cr, ci = cols[r]
            a_re = cr * m_re - ci * m_im
            a_im = cr * m_im + ci * m_re
            put3(al, (), r, B, a_re, a_im, False)
            mf[0, pl.ds(r, CH)] = jnp.where(on, 1.0, 0.0) - a_re
            mf[1, pl.ds(r, CH)] = -a_im
        sq = product(thirds(al), thirds(al))
        between(0)
        for r, a, _ in chunks():
            u_re, u_im = sq(a)
            put3(ul, (), r, B, u_re, u_im, False)
            mf[0, pl.ds(r, CH)] += u_re
            mf[1, pl.ds(r, CH)] += u_im
        cube = product(thirds(ul), thirds(al))
        between(1)
        for r, a, _ in chunks():
            c_re, c_im = cube(a)
            t_re = mf[0, pl.ds(r, CH)] - c_re
            t_im = mf[1, pl.ds(r, CH)] - c_im
            g_re = t_re * rr - t_im * ri
            g_im = t_re * ri + t_im * rr
            gf[i, pl.ds(r, CH)] = g_re
            gf[i, pl.ds(B + r, CH)] = g_im
            put3(gs, (), r, B, g_re, g_im, False)

    def put_source(i, s_re, s_im):
        gamma = source(i)
        for r, a, _ in chunks():
            x = jnp.where(diagonal_of(r, B), gamma, 0.0)
            if s_re is not None:
                x = x + s_re[a]
            put3(ss, (), r, B, x, jnp.zeros((CH, B), f32) if s_im is None else s_im[a], False)

    def lesser_left():
        t = product(thirds(gs), thirds(ss))
        for r, a, _ in chunks():
            put3(tl, (), r, B, *t(a), True)

    def lesser_of(i):
        w = product(thirds(tl), thirds(gs), True)
        for r, a, _ in chunks():
            w_re, w_im = w(a)
            wf[i, pl.ds(r, CH)] = w_re
            wf[i, pl.ds(B + r, CH)] = w_im
            put(ws, (pl.ds(r, CH),), w_re)
            put(ws, (pl.ds(B + r, CH),), w_im)

    for r, _, _ in chunks():
        mf[0, pl.ds(r, CH)] = -onsite[0, pl.ds(r, CH)]
        mf[1, pl.ds(r, CH)] = jnp.zeros((CH, B), f32)
    put_source(0, None, None)
    green_from(0, lambda stage: None)

    def forward_step(i, carry):
        kind = bk_ref[i - 1]
        v = jnp.where(kind == 0, couplings[0], jnp.where(kind == 1, couplings[1], couplings[2]))
        put(vv, (slice(None),), v)
        put(vt, (slice(None),), v.T)
        p = dot3(get(gs, both), get(vv))
        for r, a, b in chunks():
            put3(pr, (i - 1,), r, 2 * B, p[a], p[b], False)
        lesser_left()
        part = lambda j: dot3(get(vt), get(pr, i - 1, pl.ds((0, 2, 1, 3)[j] * B, B)))
        m = part(0), part(1)
        for r, a, _ in chunks():
            mf[0, pl.ds(r, CH)] = -onsite[i, pl.ds(r, CH)] - m[0][a]
            mf[1, pl.ds(r, CH)] = -m[1][a]
        lesser_of(i - 1)

        def between(stage):
            if stage == 0:
                q = dot3(get(ws, both), get(vv))
                for r, a, b in chunks():
                    put3(pr, (i - 1,), B + r, 2 * B, q[a], q[b], True)
            else:
                put_source(i, part(2), part(3))

        green_from(i, between)
        return carry

    for copy in copies[3:]:
        copy.wait()
    lax.fori_loop(1, layers + 1, forward_step, 0)
    pl.semaphore_wait(barrier, len(peers))
    lesser_left()
    lesser_of(layers)
    hf[...] = jnp.zeros_like(hf)

    def report(i, m, r, x):
        if i == layers:
            return
        x = weight * x
        for half in range(0, CH, 16):
            e = (r + half) // 16
            blocks[i, m, e // 4, e // 2 % 2, e % 2] = x[half : half + 16]

    def finish(i, last):
        h_re, h_im = hf[0].T, hf[1].T
        for r, a, _ in chunks():
            w_re = wf[i, pl.ds(r, CH)] + (hf[0, pl.ds(r, CH)] + h_re[a])
            w_im = wf[i, pl.ds(B + r, CH)] + (hf[1, pl.ds(r, CH)] - h_im[a])
            report(i, 0, r, w_re)
            report(i, 1, r, w_im)
            if not last:
                put3(ws, (), r, B, w_re, w_im, False)

    def backward(i, inner):
        from_left = lambda n: get(pr, i, pl.ds(2 * n * B, B))
        from_right = lambda n: get(pr, i, pl.ds((2 * n + 1) * B, B))
        if inner:
            q = product(from_left, thirds(gs))
        z = product(from_right, thirds(gs), True)
        finish(i + 1, False)
        if i < layers - 1:
            core_start(i + 1)
        pw = product(from_left, thirds(ws))
        if inner:
            for r, a, _ in chunks():
                put3(al, (), r, B, *q(a), False)
            grown = product(thirds(al), from_left, False, True)
        for r, a, _ in chunks():
            (p_re, p_im), (z_re, z_im) = pw(a), z(a)
            report(i, 2, r, p_re + z_re)
            report(i, 3, r, p_im + z_im)
            put3(ml, (), r, B, 0.5 * p_re + z_re, 0.5 * p_im + z_im, True)
        if inner:
            for r, a, _ in chunks():
                n_re, n_im = grown(a)
                put3(gs, (), r, B, gf[i, pl.ds(r, CH)] + n_re, gf[i, pl.ds(B + r, CH)] + n_im, False)
        h = product(thirds(ml), from_left, True, True)
        for r, a, _ in chunks():
            hf[0, pl.ds(r, CH)], hf[1, pl.ds(r, CH)] = h(a)
        if i < layers - 1:
            core_finish(i + 1)
            plane_start(i + 1)

    backward(3, True)
    for i in (2, 1, 0):
        backward(i, i > 0)
    finish(0, True)
    core_start(0)
    plane_gather(3)
    core_finish(0)
    plane_start(0)
    plane_gather(2)
    plane_gather(1)
    plane_turn(1, 3)
    plane_gather(0)
    plane_turn(0, 1)
    line_start(1, 3)
    line_start(0, 1)
    line_finish(1, 3)
    owners_above()
    line_finish(0, 1)
    owner_exchange()
    for i in range(layers):
        wait(from_core.at[i], core_sems.at[0, i])
        wait(from_x.at[i], first_sems.at[0, 0, i])
        wait(from_y.at[i], first_sems.at[0, 1, i])
    for lo, n in ((0, 1), (1, 3)):
        some = pl.ds(lo, n)
        for way in range(2):
            wait(from_second.at[some, way], second_sems.at[0, way, lo])
        wait(from_line.at[some], line_sems.at[0, lo])
    wait(many, owner_sems.at[0])


def scratch(layers):
    pair = lambda *s: [pltpu.VMEM(s, bf16), pltpu.VMEM(s, bf16)]
    full = lambda *s: pltpu.VMEM(s, f32)
    three = pair(3 * B, B)
    return (
        three + three + pair(layers, 6 * B, B) + three + three + three + three + three
        + pair(B, B) + pair(B, B)
        + [full(layers + 1, 2 * B, B)] * 2 + [full(2, B, B)] * 2
        + [
            full(layers, 4, 4, 2, 2, 16, B),
            full(layers, 4, 4, 2, 16, B),
            full(layers, 4, 4, 16, B),
            full(layers, 4, 4, 4, 8, 128),
            full(layers, 3, 4, 16, B),
            full(layers, 3, 4, 4, 8, 128),
            full(layers, 2, 4, 4, 8, 128),
            full(layers, 2, 3, 4, 8, 128),
            full(layers, 2, 4, 8, 128),
            full(layers, 7, 8, 128),
            full(layers, 8, 128),
            full(15, 8, 128),
            pltpu.SemaphoreType.DMA((2, layers)),
            pltpu.SemaphoreType.DMA((2, 2, layers)),
            pltpu.SemaphoreType.DMA((2, 2, 2)),
            pltpu.SemaphoreType.DMA((2, 2)),
            pltpu.SemaphoreType.DMA((3,)),
        ]
    )


def per_device(
    energies, momenta, energy_level, momentum_level, energy_table, momentum_table,
    onsite, broad, kdiag, fermi, couplings, bond_kind,
):
    layers = onsite.shape[0] - 1
    args = (
        energies, momenta, energy_level, momentum_level, energy_table, momentum_table,
        fermi, bond_kind, broad, kdiag, couplings, onsite,
    )
    held = [pltpu.VMEM(x.shape, x.dtype) for x in args[8:]]
    owned = pl.pallas_call(
        sweeps,
        out_shape=jax.ShapeDtypeStruct((4, 2, 8, B), f32),
        in_specs=[pl.BlockSpec(memory_space=pltpu.SMEM)] * 8 + [pl.BlockSpec(memory_space=pl.ANY)] * 4,
        out_specs=pl.BlockSpec(memory_space=pl.ANY),
        scratch_shapes=held + [pltpu.SemaphoreType.DMA((5,))] + scratch(layers),
        compiler_params=pltpu.CompilerParams(
            vmem_limit_bytes=62 << 20, collective_id=0, has_side_effects=True
        ),
        name="sweeps",
    )(*args).reshape(4, 16, B)
    return owned[None, :2], owned[None, 2:]


def solution(mesh):
    rep = P()
    both = P(("energy", "layer"))
    return jax.shard_map(
        per_device,
        mesh=mesh,
        in_specs=(both, P("kpt"), both, P("kpt"), rep, rep, rep, rep, rep, rep, rep, rep),
        out_specs=(P("layer", None, "energy", None), P("layer", None, "energy", None)),
        check_vma=False,
    )
```
